16 devices in a mesh: model: 2 (over z), sub: 2 (over y), data: 4 (over x, core).
Axes of the slice: x: 2, y: 2, z: 2, core: 2. Of those that a mesh axis runs over, the one named last changes fastest.
Arguments:
- images: bfloat16 [16, 576, 384], P(('model', 'sub', 'data'))
- targets: bfloat16 [16, 576, 384], P(('model', 'sub', 'data'))
- w_in: float32 [16, 384, 1536], replicated
- w_out: float32 [16, 1536, 384], replicated
Outputs:
- output 1: float32 [16, 384, 1536], replicated
- output 2: float32 [16, 1536, 384], replicated
- output 3: float32 [], replicated
All inputs are finite; a program needn't handle non-finite values.
Results may differ from the reference program's by a relative error of at most 0.00699408.
Values are sent between devices in bfloat16 or wider.
A program may use at most 1 GiB of HBM per device.

```python
import jax
import jax.numpy as jnp
import math
from jax import lax

D = 384
FF = 1536
SEQ = 576
LAYERS = 16
IMGS_DEV = 1
DEVICES = 16
IMAGES = IMGS_DEV * DEVICES
TOKENS = IMAGES * SEQ
BLOCK_ROWS = IMGS_DEV * SEQ
INV_COUNT = 1.0 / (TOKENS * D)
RHO_REL = 0.1
RADIUS = RHO_REL * math.sqrt(LAYERS * FF + D)
LEARN_RATE = 8.0
SQRT_HALF = 0.7071067811865476
INV_SQRT_2PI = 0.3989422804014327


def setup_inputs(seed: int = 0) -> dict:
    root_key = jax.random.key(seed)
    subkeys = jax.random.split(root_key, 8)
    img_shift = 0.8 * jax.random.normal(subkeys[0], (IMAGES, 1, D), jnp.float32)
    img_gain = jnp.exp(0.3 * jax.random.normal(subkeys[1], (IMAGES, 1, 1), jnp.float32))
    images = jax.random.normal(subkeys[2], (IMAGES, SEQ, D), jnp.float32) * img_gain + img_shift
    tgt_shift = 0.5 * jax.random.normal(subkeys[3], (1, 1, D), jnp.float32) + 0.8 * jax.random.normal(subkeys[4], (IMAGES, 1, D), jnp.float32)
    targets = jax.random.normal(subkeys[5], (IMAGES, SEQ, D), jnp.float32) + tgt_shift
    w_in = jax.random.normal(subkeys[6], (LAYERS, D, FF), jnp.float32) * D ** -0.5
    w_out = jax.random.normal(subkeys[7], (LAYERS, FF, D), jnp.float32) * (FF * LAYERS) ** -0.5
    return {'images': images.astype(jnp.bfloat16), 'targets': targets.astype(jnp.bfloat16), 'w_in': w_in, 'w_out': w_out}


def gelu_fn(pre_act):
    return 0.5 * pre_act * (1.0 + lax.erf(pre_act * SQRT_HALF))


def gelu_slope(pre_act):
    cdf_part = 0.5 * (1.0 + lax.erf(pre_act * SQRT_HALF))
    return cdf_part + pre_act * INV_SQRT_2PI * jnp.exp(-0.5 * pre_act * pre_act)


def layer_forward(hidden, weights):
    w_in_l, w_out_l = weights
    pre_act = jnp.dot(hidden, w_in_l, preferred_element_type=jnp.float32).astype(jnp.bfloat16)
    post_act = gelu_fn(pre_act.astype(jnp.float32)).astype(jnp.bfloat16)
    mlp_out = jnp.dot(post_act, w_out_l, preferred_element_type=jnp.float32)
    new_hidden = (hidden.astype(jnp.float32) + mlp_out).astype(jnp.bfloat16)
    return new_hidden, (hidden, pre_act, post_act)


def layer_backward(d_hidden, inputs_l):
    hidden, pre_act, post_act, w_in_l, w_out_l = inputs_l
    grad_out = jnp.dot(post_act.T, d_hidden, preferred_element_type=jnp.float32)
    d_act = jnp.dot(d_hidden, w_out_l.T, preferred_element_type=jnp.float32)
    d_pre = (d_act * gelu_slope(pre_act.astype(jnp.float32))).astype(jnp.bfloat16)
    grad_in = jnp.dot(hidden.T, d_pre, preferred_element_type=jnp.float32)
    d_prev = (d_hidden.astype(jnp.float32) + jnp.dot(d_pre, w_in_l.T, preferred_element_type=jnp.float32)).astype(jnp.bfloat16)
    return d_prev, (grad_in, grad_out)


def block_grads(x_rows, y_rows, w_in_bf, w_out_bf):
    top_hidden, saved_acts = lax.scan(layer_forward, x_rows, (w_in_bf, w_out_bf))
    resid_err = top_hidden.astype(jnp.float32) - y_rows.astype(jnp.float32)
    d_top = (resid_err * INV_COUNT).astype(jnp.bfloat16)
    hiddens, pre_acts, post_acts = saved_acts
    _, grads = lax.scan(layer_backward, d_top, (hiddens, pre_acts, post_acts, w_in_bf, w_out_bf), reverse=True)
    return 0.5 * jnp.sum(resid_err * resid_err), grads[0], grads[1]


def full_grads(images, targets, w_in_bf, w_out_bf):
    x_blocks = images.reshape(DEVICES, BLOCK_ROWS, D)
    y_blocks = targets.reshape(DEVICES, BLOCK_ROWS, D)

    def accumulate(totals, block_pair):
        loss_blk, gin_blk, gout_blk = block_grads(block_pair[0], block_pair[1], w_in_bf, w_out_bf)
        return (totals[0] + loss_blk, totals[1] + gin_blk, totals[2] + gout_blk), None

    init_carry = (jnp.zeros((), jnp.float32), jnp.zeros((LAYERS, D, FF), jnp.float32), jnp.zeros((LAYERS, FF, D), jnp.float32))
    totals, _ = lax.scan(accumulate, init_carry, (x_blocks, y_blocks))
    return totals


def reference(images, targets, w_in, w_out):
    _, grad_in, grad_out = full_grads(images, targets, w_in.astype(jnp.bfloat16), w_out.astype(jnp.bfloat16))
    grad_norm = jnp.sqrt(jnp.sum(grad_in * grad_in) + jnp.sum(grad_out * grad_out))
    step_scale = RADIUS / grad_norm
    pert_in = (w_in + step_scale * grad_in).astype(jnp.bfloat16)
    pert_out = (w_out + step_scale * grad_out).astype(jnp.bfloat16)
    loss_sum, grad2_in, grad2_out = full_grads(images, targets, pert_in, pert_out)
    return (w_in - LEARN_RATE * grad2_in, w_out - LEARN_RATE * grad2_out, loss_sum * INV_COUNT)
```

```python
import functools
import math

import jax
import jax.numpy as jnp
from jax import lax
from jax.experimental import pallas as pl
from jax.experimental.pallas import tpu as pltpu
from jax.sharding import PartitionSpec as P

MESH = pl.DeviceIdType.MESH
RHO_REL = 0.1
LEARN_RATE = 8.0
SQRT_HALF = 0.7071067811865476
INV_SQRT_2PI = 0.3989422804014327

CHIPS = 8
LAYERS = 16
D = 384
F = 1536
T = 576
ROWS = CHIPS * T
FT = 768
KB_ROWS = 512
KB_FT = 512

f32, bf16 = jnp.float32, jnp.bfloat16
NN = (((1,), (0,)), ((), ()))
NT = (((1,), (1,)), ((), ()))
V = pl.BlockSpec(memory_space=pltpu.VMEM)
ANY = pl.BlockSpec(memory_space=pl.ANY)
DMA = pltpu.SemaphoreType.DMA


def dot(a, b, dims=NN):
    return lax.dot_general(a, b, dims, preferred_element_type=f32)


def cdf(x):
    return 0.5 * (1.0 + lax.erf(x * SQRT_HALF))


def slope_tail(x):
    return x * INV_SQRT_2PI * jnp.exp(-0.5 * x * x)


class Place:
    def __init__(self):
        self.z, self.y, data = lax.axis_index("model"), lax.axis_index("sub"), lax.axis_index("data")
        self.x, self.core = data // 2, data % 2
        self.chip = self.z * 4 + self.y * 2 + self.x
        self.coords = (self.x, self.y, self.z)

    def device(self, chip, core):
        return (chip // 4, (chip // 2) % 2, (chip % 2) * 2 + core)

    def partner(self):
        return self.device(self.chip, 1 - self.core)

    def flipped(self, dims):
        x, y, z = ((1 - v) if d in dims else v for d, v in enumerate(self.coords))
        return z * 4 + y * 2 + x

    def neighbour(self, dim):
        return self.device(self.flipped((dim,)), self.core)

    def same_core_peers(self):
        return [self.device(self.flipped(s), self.core) for s in SUBSETS[1:]]

    def all_peers(self):
        return self.same_core_peers() + [self.device(self.flipped(s), 1 - self.core) for s in SUBSETS]


SUBSETS = ((), (0,), (1,), (0, 1), (2,), (0, 2), (1, 2), (0, 1, 2))


def meet(peers):
    barrier = pltpu.get_barrier_semaphore()
    for peer in peers:
        pl.semaphore_signal(barrier, inc=1, device_id=peer, device_id_type=MESH)
    pl.semaphore_wait(barrier, len(peers))


def remote(src, dst, send_sem, recv_sem, device):
    return pltpu.make_async_remote_copy(
        src_ref=src, dst_ref=dst, send_sem=send_sem, recv_sem=recv_sem, device_id=device, device_id_type=MESH
    )


class Gather:
    def __init__(self, at, tensors, send, recv, pair_send, pair_recv):
        self.at, self.tensors = at, tensors
        self.send, self.recv, self.pair_send, self.pair_recv = send, recv, pair_send, pair_recv
        self.pairs, self.copies = [], {}

    def messages(self, dim):
        a, b = (dim - 1) % 3, (dim - 2) % 3
        return [(dim, ()), (a, ()), (b, ()), (a, (a,)), (b, (b,)), (b, (a,)), (b, (a, b))]

    def make(self, part, flips, send, recv, device):
        layer = self.at.flipped(flips) * 2 + self.at.core
        out = []
        for i, (own, slots) in enumerate(self.tensors):
            n = slots.shape[1] // 3
            rows = pl.ds(part * n, n)
            dst = slots.at[layer, rows, :]
            src = own.at[rows, :] if not flips else dst
            out.append(remote(src, dst, send.at[i], recv.at[i], device))
        return out

    def link(self, dim, slot):
        if (dim, slot) not in self.copies:
            part, flips = self.messages(dim)[slot]
            self.copies[dim, slot] = self.make(
                part, flips, self.send.at[dim, slot], self.recv.at[dim, slot], self.at.neighbour(dim)
            )
        return self.copies[dim, slot]

    def hand_over(self, part, flips):
        i = len(self.pairs)
        copies = self.make(part, flips, self.pair_send.at[i], self.pair_recv.at[i], self.at.partner())
        for c in copies:
            c.start()
        self.pairs.append(copies)

    def start(self):
        for slot in range(3):
            for dim in range(3):
                for c in self.link(dim, slot):
                    c.start()
        for part in range(3):
            self.hand_over(part, ())

    def run(self):
        relay = {0: (3, 4), 1: (5,), 3: (6,)}
        for slot in range(7):
            for dim in range(3):
                for c in self.link(dim, slot):
                    c.wait_recv()
            for later in relay.get(slot, ()):
                for dim in range(3):
                    for c in self.link(dim, later):
                        c.start()
            for dim in range(3):
                part, flips = self.messages(dim)[slot]
                self.hand_over(part, tuple(sorted(set(flips) ^ {dim})))
        for copies in self.pairs:
            for c in copies:
                c.wait_recv()

    def finish(self):
        for copies in [*self.pairs, *self.copies.values()]:
            for c in copies:
                c.wait_send()


GATHER_SEMS = [DMA((3, 7, 2)), DMA((3, 7, 2)), DMA((24, 2)), DMA((24, 2))]


def local_kernel(perturbed, inv_count, *refs):
    if perturbed:
        (x_ref, y_ref, wi_own, wo_own, h_out, d_out, pi_out, po_out, u_hbm, loss_out,
         wi, wo, hs, ds, mid, acc, us, hsend, hrecv, dsend, drecv, usem, wsem,
         gs, gr, ps, pr, lbuf, lsend, lrecv) = refs
    else:
        (x_ref, y_ref, wi_hbm, wo_hbm, h_out, d_out, pi_out, po_out, u_hbm,
         wi, wo, hs, ds, mid, acc, us, hsend, hrecv, dsend, drecv, usem, wsem,
         si, so, ssem) = refs
    at = Place()
    me = at.chip

    def fetch(layer):
        slot = layer % 2
        return (pltpu.make_async_copy(wi_hbm.at[layer], si.at[slot], ssem.at[slot, 0]),
                pltpu.make_async_copy(wo_hbm.at[layer], so.at[slot], ssem.at[slot, 1]))

    own = me * 2 + at.core
    if perturbed:
        loads = [pltpu.make_async_copy(wi_own, wi.at[own], wsem.at[0]), pltpu.make_async_copy(wo_own, wo.at[own], wsem.at[1])]
        for c in loads:
            c.start()
        meet(at.all_peers())
        for c in loads:
            c.wait()
        gather = Gather(at, [(wi.at[own], wi), (wo.at[own], wo)], gs, gr, ps, pr)
        gather.start()
        gather.run()
    else:
        for layer in range(2):
            for c in fetch(layer):
                c.start()
        meet(at.same_core_peers())

    def send(k, src, dst, send_sem, recv_sem):
        @pl.when(k == me)
        def _():
            pltpu.make_async_copy(src, dst.at[me], recv_sem.at[me]).start()

        @pl.when(k != me)
        def _():
            remote(src, dst.at[me], send_sem.at[k], recv_sem.at[me], at.device(k, at.core)).start()

    def layer_forward(layer, hidden, between):
        slot = layer % 2

        @pl.when(jnp.logical_and(layer >= 4, layer < LAYERS))
        def _():
            pltpu.make_async_copy(us.at[slot], u_hbm.at[layer - 2], usem.at[slot]).wait()

        if not perturbed:
            for c in fetch(layer):
                c.wait()
        for j in range(0, F, FT):
            cols = pl.ds(j, FT)
            if perturbed:
                a_w, b_w = wi[layer, :, cols], wo[layer, cols, :]
            else:
                a_w, b_w = si[slot, :, cols].astype(bf16), so[slot, cols, :].astype(bf16)
                wi[layer, :, cols] = a_w
                wo[layer, cols, :] = b_w
            pre = dot(hidden, a_w).astype(bf16)
            us[slot, :, cols] = pre
            pre = pre.astype(f32)
            part = dot((pre * cdf(pre)).astype(bf16), b_w)
            if j == 0:
                acc[...] = part
                between()
            else:
                acc[...] += part

        @pl.when(jnp.logical_and(layer >= 2, layer < LAYERS - 2))
        def _():
            pltpu.make_async_copy(us.at[slot], u_hbm.at[layer], usem.at[slot]).start()

        if not perturbed:
            @pl.when(layer < LAYERS - 2)
            def _():
                for c in fetch(layer + 2):
                    c.start()
        return (hidden.astype(f32) + acc[...]).astype(bf16)

    hs[0] = x_ref[...]

    def pair_forward(k, carry):
        mid[...] = layer_forward(2 * k, hs[k], lambda: send(k, hs.at[k], h_out, hsend, hrecv))
        hs[k + 1] = layer_forward(2 * k + 1, mid[...], lambda: None)
        return carry

    lax.fori_loop(0, CHIPS, pair_forward, 0)

    for i, (src, dst) in enumerate(((wi, pi_out), (wo, po_out))):
        pltpu.make_async_copy(src.at[pl.ds(2 * me, 2)], dst, wsem.at[i]).start()

    resid = hs[CHIPS].astype(f32) - y_ref[...].astype(f32)
    ds[CHIPS - 1] = (resid * inv_count).astype(bf16)
    if perturbed:
        mine = me * 2 + at.core
        lbuf[mine] = jnp.broadcast_to(0.5 * jnp.sum(resid * resid, axis=(0, 1), keepdims=True), (8, 128))

    def layer_backward(layer, cot, between):
        slot = layer % 2

        @pl.when(layer < LAYERS - 2)
        def _():
            pltpu.make_async_copy(u_hbm.at[layer], us.at[slot], usem.at[slot]).wait()

        for j in range(0, F, FT):
            cols = pl.ds(j, FT)
            pre = us[slot, :, cols].astype(f32)
            err = (dot(cot, wo[layer, cols, :], NT) * (cdf(pre) + slope_tail(pre))).astype(bf16)
            part = dot(err, wi[layer, :, cols], NT)
            if j == 0:
                acc[...] = part
                between()
            else:
                acc[...] += part

        @pl.when(layer >= 4)
        def _():
            pltpu.make_async_copy(u_hbm.at[layer - 2], us.at[slot], usem.at[slot]).start()

        return (cot.astype(f32) + acc[...]).astype(bf16)

    def pair_backward(i, carry):
        k = CHIPS - 1 - i
        mid[...] = layer_backward(2 * k + 1, ds[k], lambda: send(k, ds.at[k], d_out, dsend, drecv))
        ds[k - 1] = layer_backward(2 * k, mid[...], lambda: None)
        return carry

    if perturbed:
        def loss_copy(i, peer):
            return remote(lbuf.at[mine], lbuf.at[mine], lsend.at[i], lrecv.at[mine], peer)

        for i, peer in enumerate(at.all_peers()):
            loss_copy(i, peer).start()

    lax.fori_loop(0, CHIPS - 1, pair_backward, 0)
    send(0, ds.at[0], d_out, dsend, drecv)

    for i, (src, dst) in enumerate(((wi, pi_out), (wo, po_out))):
        pltpu.make_async_copy(src.at[pl.ds(2 * me, 2)], dst, wsem.at[i]).wait()

    def drain(k, carry):
        @pl.when(k != me)
        def _():
            remote(hs.at[0], h_out.at[k], hsend.at[k], hrecv.at[k], at.device(k, at.core)).wait_send()
            remote(ds.at[0], d_out.at[k], dsend.at[k], drecv.at[k], at.device(k, at.core)).wait_send()

        pltpu.make_async_copy(hs.at[0], h_out.at[k], hrecv.at[k]).wait()
        pltpu.make_async_copy(ds.at[0], d_out.at[k], drecv.at[k]).wait()
        return carry

    lax.fori_loop(0, CHIPS, drain, 0)

    if perturbed:
        for i, peer in enumerate(at.all_peers()):
            loss_copy(i, peer).wait_send()

        def gathered(i, carry):
            @pl.when(i != mine)
            def _():
                remote(lbuf.at[i], lbuf.at[i], lsend.at[0], lrecv.at[i], at.partner()).wait_recv()

            return carry

        lax.fori_loop(0, LAYERS, gathered, 0)
        total = lbuf[0]
        for i in range(1, LAYERS):
            total = total + lbuf[i]
        loss_out[...] = total * inv_count
        gather.finish()


def owner_kernel(perturbed, radius, *refs):
    if perturbed:
        (h_ref, d_ref, a_ref, b_ref, wi_hbm, wo_hbm, wi_out, wo_out,
         gi, go, u_low, a_low, acc, ri, ro, wi, wo, wsem, xsend, xrecv, gs, gr, ps, pr) = refs
    else:
        (h_ref, d_ref, a_ref, b_ref, wi_hbm, wo_hbm, wi_out, wo_out,
         gi, go, u_low, a_low, acc, ri, ro, wi, wo, wsem, xsend, xrecv, sbuf, ssend, srecv) = refs
    at = Place()
    mine = at.chip * 2 + at.core
    loads = [pltpu.make_async_copy(wi_hbm.at[mine], wi, wsem.at[0]), pltpu.make_async_copy(wo_hbm.at[mine], wo, wsem.at[1])]
    for c in loads:
        c.start()

    def block(i, carry):
        rows = pl.ds(pl.multiple_of(i * KB_ROWS, KB_ROWS), KB_ROWS)
        first = i == 0

        def add(ref, which, cols, value):
            ref[which, :, cols] = jnp.where(first, 0.0, ref[which, :, cols]) + value

        h_low = h_ref[rows, :]
        d_top = d_ref[rows, :]
        acc[...] = h_low.astype(f32)
        for j in range(0, F, KB_FT):
            cols = pl.ds(j, KB_FT)
            pre = dot(h_low, a_ref[0, :, cols]).astype(bf16)
            u_low[:, cols] = pre
            pre = pre.astype(f32)
            post = (pre * cdf(pre)).astype(bf16)
            a_low[:, cols] = post
            acc[...] += dot(post, b_ref[0, cols, :])
        h_mid = acc[...].astype(bf16)
        d_top_t, h_mid_t = d_top.T, h_mid.T
        acc[...] = d_top.astype(f32)
        for j in range(0, F, KB_FT):
            cols = pl.ds(j, KB_FT)
            pre = dot(h_mid, a_ref[1, :, cols]).astype(bf16).astype(f32)
            half = cdf(pre)
            post = (pre * half).astype(bf16)
            err = (dot(d_top, b_ref[1, cols, :], NT) * (half + slope_tail(pre))).astype(bf16)
            add(go, 1, cols, dot(d_top_t, post))
            add(gi, 1, cols, dot(h_mid_t, err))
            acc[...] += dot(err, a_ref[1, :, cols], NT)
        d_mid = acc[...].astype(bf16)
        d_mid_t, h_low_t = d_mid.T, h_low.T
        for j in range(0, F, KB_FT):
            cols = pl.ds(j, KB_FT)
            pre = u_low[:, cols].astype(f32)
            err = (dot(d_mid, b_ref[0, cols, :], NT) * (cdf(pre) + slope_tail(pre))).astype(bf16)
            add(go, 0, cols, dot(d_mid_t, a_low[:, cols]))
            add(gi, 0, cols, dot(h_low_t, err))
        return carry

    lax.fori_loop(0, ROWS // KB_ROWS, block, 0)
    meet([at.partner()] + [at.neighbour(d) for d in range(3)] if perturbed else at.all_peers())

    other = 1 - at.core
    swap = [remote(gi.at[other], ri, xsend.at[0], xrecv.at[0], at.partner()),
            remote(go.at[other], ro, xsend.at[1], xrecv.at[1], at.partner())]
    for c in swap:
        c.start()
    for c in loads:
        c.wait()

    def squares(value, total):
        sq = value * value
        for r in range(0, sq.shape[0], 8):
            for q in range(0, sq.shape[1], 128):
                total = total + sq[r:r + 8, q:q + 128]
        return total

    R, C = 16, 128

    def sum_in(i, total):
        rows = pl.ds(pl.multiple_of(i * R, R), R)
        g = gi[at.core, rows, :] + ri[rows, :]
        if perturbed:
            wi[rows, :] = wi[rows, :] - LEARN_RATE * g
            return total
        ri[rows, :] = g
        return squares(g, total)

    def sum_out(i, total):
        cols = pl.ds(pl.multiple_of(i * C, C), C)
        g = go[at.core, :, cols] + ro[:, cols]
        if perturbed:
            wo[cols, :] = wo[cols, :] - LEARN_RATE * g.T
            return total
        ro[:, cols] = g
        return squares(g, total)

    total = jnp.zeros((8, 128), f32)
    swap[0].wait_recv()
    total = lax.fori_loop(0, D // R, sum_in, total)
    swap[1].wait_recv()
    total = lax.fori_loop(0, F // C, sum_out, total)

    if perturbed:
        gather = Gather(at, [(wi, wi_out), (wo, wo_out)], gs, gr, ps, pr)
        keep = [pltpu.make_async_copy(wi, wi_out.at[mine], wsem.at[0]), pltpu.make_async_copy(wo, wo_out.at[mine], wsem.at[1])]
        gather.start()
        for c in keep:
            c.start()
        gather.run()
        gather.finish()
        for c in keep:
            c.wait()
    else:
        sbuf[mine] = total
        peers = at.all_peers()
        sends = [remote(sbuf.at[mine], sbuf.at[mine], ssend.at[i], srecv.at[mine], p) for i, p in enumerate(peers)]
        for c in sends:
            c.start()

        def gathered(i, carry):
            @pl.when(i != mine)
            def _():
                remote(sbuf.at[i], sbuf.at[i], ssend.at[0], srecv.at[i], at.partner()).wait_recv()

            return carry

        lax.fori_loop(0, LAYERS, gathered, 0)
        total = sbuf[0]
        for i in range(1, LAYERS):
            total = total + sbuf[i]
        scale = radius / jnp.sqrt(jnp.sum(total, axis=(0, 1), keepdims=True))

        def perturb_in(i, carry):
            rows = pl.ds(pl.multiple_of(i * R, R), R)
            wi_out[rows, :] = (wi[rows, :] + scale * ri[rows, :]).astype(bf16)
            return carry

        def perturb_out(i, carry):
            cols = pl.ds(pl.multiple_of(i * C, C), C)
            wo_out[cols, :] = (wo[cols, :] + scale * ro[:, cols].T).astype(bf16)
            return carry

        lax.fori_loop(0, D // R, perturb_in, 0)
        lax.fori_loop(0, F // C, perturb_out, 0)
        for c in sends:
            c.wait_send()
    for c in swap:
        c.wait_send()


def local_pass(perturbed, inv_count, x, y, wi, wo):
    shapes = [((CHIPS, T, D), bf16), ((CHIPS, T, D), bf16), ((2, D, F), bf16), ((2, F, D), bf16), ((LAYERS, T, F), bf16)]
    specs = [ANY] * 5
    scratch = [
        pltpu.VMEM((LAYERS, D, F), bf16), pltpu.VMEM((LAYERS, F, D), bf16),
        pltpu.VMEM((CHIPS + 1, T, D), bf16), pltpu.VMEM((CHIPS, T, D), bf16),
        pltpu.VMEM((T, D), bf16), pltpu.VMEM((T, D), f32), pltpu.VMEM((2, T, F), bf16),
        DMA((CHIPS,)), DMA((CHIPS,)), DMA((CHIPS,)), DMA((CHIPS,)), DMA((2,)), DMA((2,)),
    ]
    if perturbed:
        shapes.append(((8, 128), f32))
        specs.append(V)
        scratch += [*GATHER_SEMS, pltpu.VMEM((LAYERS, 8, 128), f32), DMA((15,)), DMA((LAYERS,))]
    else:
        scratch += [pltpu.VMEM((2, D, F), f32), pltpu.VMEM((2, F, D), f32), DMA((2, 2))]
    return pl.pallas_call(
        functools.partial(local_kernel, perturbed, inv_count),
        out_shape=[jax.ShapeDtypeStruct(*s) for s in shapes],
        in_specs=[V, V, ANY, ANY],
        out_specs=specs,
        scratch_shapes=scratch,
        compiler_params=pltpu.CompilerParams(
            collective_id=2 if perturbed else 0, has_side_effects=True, vmem_limit_bytes=67043328),
        name="local_perturbed" if perturbed else "local",
    )(x, y, wi, wo)


def owner_pass(perturbed, radius, h, d, a, b, wi, wo):
    if perturbed:
        shapes = [((LAYERS, D, F), f32), ((LAYERS, F, D), f32)]
        tail = GATHER_SEMS
    else:
        shapes = [((D, F), bf16), ((F, D), bf16)]
        tail = [pltpu.VMEM((LAYERS, 8, 128), f32), DMA((15,)), DMA((LAYERS,))]
    scratch = [
        pltpu.VMEM((2, D, F), f32), pltpu.VMEM((2, D, F), f32),
        pltpu.VMEM((KB_ROWS, F), bf16), pltpu.VMEM((KB_ROWS, F), bf16), pltpu.VMEM((KB_ROWS, D), f32),
        pltpu.VMEM((D, F), f32), pltpu.VMEM((D, F), f32), pltpu.VMEM((D, F), f32), pltpu.VMEM((F, D), f32),
        DMA((2,)), DMA((2,)), DMA((2,)), *tail,
    ]
    return pl.pallas_call(
        functools.partial(owner_kernel, perturbed, radius),
        out_shape=[jax.ShapeDtypeStruct(*s) for s in shapes],
        in_specs=[V, V, V, V, ANY, ANY],
        out_specs=[ANY, ANY] if perturbed else [V, V],
        scratch_shapes=scratch,
        compiler_params=pltpu.CompilerParams(
            collective_id=3 if perturbed else 1, has_side_effects=True, vmem_limit_bytes=60 * 2**20),
        name="owner_perturbed" if perturbed else "owner",
    )(h.reshape(ROWS, D), d.reshape(ROWS, D), a, b, wi, wo)


def solution(mesh):
    mesh_axes = tuple(mesh.axis_names)
    dev_count = math.prod([mesh.shape[axis_name] for axis_name in mesh_axes])
    batch_spec = P(mesh_axes, None, None)

    def local_step(images, targets, w_in, w_out):
        layers, model_dim, hidden_dim = w_in.shape
        inv_count = 1.0 / (images.shape[0] * images.shape[1] * dev_count * model_dim)
        radius = RHO_REL * math.sqrt(layers * hidden_dim + model_dim)
        x, y = images.reshape(T, D), targets.reshape(T, D)
        h, d, a, b, _ = local_pass(False, inv_count, x, y, w_in, w_out)
        pert_in, pert_out = owner_pass(False, radius, h, d, a, b, w_in, w_out)
        h, d, a, b, _, loss = local_pass(True, inv_count, x, y, pert_in, pert_out)
        new_in, new_out = owner_pass(True, radius, h, d, a, b, w_in, w_out)
        return new_in, new_out, loss[0, 0]

    return jax.shard_map(local_step, mesh=mesh, in_specs=(batch_spec, batch_spec, P(), P()), out_specs=(P(), P(), P()), check_vma=False)
```

```python
import functools
import math

import jax
import jax.numpy as jnp
from jax import lax
from jax.experimental import pallas as pl
from jax.experimental.pallas import tpu as pltpu
from jax.sharding import PartitionSpec as P

MESH = pl.DeviceIdType.MESH
RHO_REL = 0.1
LEARN_RATE = 8.0
SQRT_HALF = 0.7071067811865476
INV_SQRT_2PI = 0.3989422804014327

CHIPS = 8
LAYERS = 16
D = 384
F = 1536
T = 576
ROWS = CHIPS * T
FT = 768
KB_ROWS = 768
KB_FT = 256
KEPT = 8
VMEM_LIMIT = 67043328

f32, bf16 = jnp.float32, jnp.bfloat16
NN = (((1,), (0,)), ((), ()))
NT = (((1,), (1,)), ((), ()))
V = pl.BlockSpec(memory_space=pltpu.VMEM)
ANY = pl.BlockSpec(memory_space=pl.ANY)
DMA = pltpu.SemaphoreType.DMA


def dot(a, b, dims=NN):
    return lax.dot_general(a, b, dims, preferred_element_type=f32)


def cdf(x):
    return 0.5 * (1.0 + lax.erf(x * SQRT_HALF))


def slope_tail(x):
    return x * INV_SQRT_2PI * jnp.exp(-0.5 * x * x)


class Place:
    def __init__(self):
        self.z, self.y, data = lax.axis_index("model"), lax.axis_index("sub"), lax.axis_index("data")
        self.x, self.core = data // 2, data % 2
        self.chip = self.z * 4 + self.y * 2 + self.x
        self.mine = self.chip * 2 + self.core

    def across(self, t):
        x, y, z = (self.x + t) % 2, (self.y + t // 2) % 2, (self.z + t // 4) % 2
        return z * 4 + y * 2 + x

    def device(self, chip, core):
        return (chip // 4, (chip // 2) % 2, (chip % 2) * 2 + core)

    def partner(self):
        return self.device(self.chip, 1 - self.core)

    def peer(self, i):
        return self.device(self.across(i // 2), (self.core + i) % 2)


def bit(dim):
    return 1 + dim + dim * (dim - 1) // 2


def each(first, last, body):
    def step(i, carry):
        body(i)
        return carry

    lax.fori_loop(first, last, step, 0)


def meet(at):
    barrier = pltpu.get_barrier_semaphore()
    each(1, 16, lambda i: pl.semaphore_signal(barrier, inc=1, device_id=at.peer(i), device_id_type=MESH))
    pl.semaphore_wait(barrier, 15)


def remote(src, dst, send_sem, recv_sem, device):
    return pltpu.make_async_remote_copy(
        src_ref=src, dst_ref=dst, send_sem=send_sem, recv_sem=recv_sem, device_id=device, device_id_type=MESH
    )


class Gather:
    MESSAGES = ((0, ()), (1, ()), (2, ()), (1, (1,)), (2, (2,)), (2, (1,)), (2, (1, 2)))

    def __init__(self, at, tensors, send, recv, pair_send, pair_recv):
        self.at, self.tensors = at, tensors
        self.sems = (send, recv, pair_send, pair_recv)

    def make(self, i, part, own, chip, send, recv, device):
        ref, slots = self.tensors[i]
        n = slots.shape[1] // 3
        rows = pl.ds(pl.multiple_of(part * n, n), n)
        dst = slots.at[chip * 2 + self.at.core, rows, :]
        return remote(ref.at[rows, :] if own else dst, dst, send, recv, device)

    def parts(self, dim, slot):
        back, turns = self.MESSAGES[slot]
        t = 0
        for o in turns:
            t = t + bit((dim + 3 - o) % 3)
        return (dim + 3 - back) % 3, t

    def link(self, i, dim, slot):
        part, t = self.parts(dim, slot)
        send, recv, _, _ = self.sems
        return self.make(i, part, slot < 3, self.at.across(t) if slot >= 3 else self.at.chip, send.at[dim, slot, i],
                         recv.at[dim, slot, i], self.at.device(self.at.across(bit(dim)), self.at.core))

    def pair(self, i, part, own, chip, index):
        _, _, send, recv = self.sems
        return self.make(i, part, own, chip, send.at[index, i], recv.at[index, i], self.at.partner())

    def start(self):
        for slot in range(3):
            for i in range(2):
                each(0, 3, lambda dim: self.link(i, dim, slot).start())
        for i in range(2):
            each(0, 3, lambda part: self.pair(i, part, True, self.at.chip, part).start())

    def run(self):
        turn = {0: (3, 1), 1: (5, 1), 3: (6, 1)}
        for slot in range(7):
            for i in range(2):
                def got(dim):
                    self.link(i, dim, slot).wait_recv()
                    if slot in turn:
                        later, step = turn[slot]
                        self.link(i, (dim + step) % 3, later).start()
                    part, t = self.parts(dim, slot)
                    self.pair(i, part, False, self.at.across(t + bit(dim)), 3 + slot * 3 + dim).start()

                each(0, 3, got)
            if slot == 0:
                for i in range(2):
                    each(0, 3, lambda dim: self.link(i, dim, 4).start())
        for i in range(2):
            each(0, 24, lambda index: self.pair(i, 0, False, self.at.chip, index).wait_recv())

    def finish(self):
        for i in range(2):
            each(0, 24, lambda index: self.pair(i, 0, False, self.at.chip, index).wait_send())
            for slot in range(7):
                each(0, 3, lambda dim: self.link(i, dim, slot).wait_send())


GATHER_SEMS = [DMA((3, 7, 2)), DMA((3, 7, 2)), DMA((24, 2)), DMA((24, 2))]


def pass_kernel(perturbed, inv_count, radius, *refs):
    if perturbed:
        (x_ref, y_ref, wi_hbm, wo_hbm, pi_own, po_own, wi_out, wo_out, wbi, wbo, u_hbm, loss_out,
         bi, bo, hs, ds, acc, us, hg, dg, gi, go, ri, ro,
         hsend, hrecv, dsend, drecv, usem, bsem, wsem, xsend, xrecv, sbuf, ssend, srecv,
         wi, wo, as_, ar, aps, apr, gs, gr, gps, gpr) = refs
    else:
        (x_ref, y_ref, wi_hbm, wo_hbm, wi_out, wo_out, u_hbm,
         bi, bo, hs, ds, acc, us, hg, dg, gi, go, ri, ro,
         hsend, hrecv, dsend, drecv, usem, bsem, wsem, xsend, xrecv, sbuf, ssend, srecv,
         si, so, fsem) = refs
    at = Place()
    me = at.chip
    mine = at.mine

    def fetch32(layer, slot):
        return (pltpu.make_async_copy(wi_hbm.at[layer], si.at[slot], fsem.at[slot, 0]),
                pltpu.make_async_copy(wo_hbm.at[layer], so.at[slot], fsem.at[slot, 1]))

    def fetch16(layer, slot):
        return (pltpu.make_async_copy(wbi.at[layer], bi.at[slot], bsem.at[slot, 0]),
                pltpu.make_async_copy(wbo.at[layer], bo.at[slot], bsem.at[slot, 1]))

    fetch = fetch16 if perturbed else fetch32

    def start(copies):
        for c in copies:
            c.start()

    def wait(copies):
        for c in copies:
            c.wait()

    own_w = [pltpu.make_async_copy(wi_hbm.at[mine], wi if perturbed else si.at[0], wsem.at[0]),
             pltpu.make_async_copy(wo_hbm.at[mine], wo if perturbed else so.at[0], wsem.at[1])]
    if perturbed:
        keep = [pltpu.make_async_copy(pi_own, wbi.at[mine], wsem.at[2]), pltpu.make_async_copy(po_own, wbo.at[mine], wsem.at[3])]
        start(keep)
        start(own_w)
        meet(at)
        spread = Gather(at, [(pi_own, wbi), (po_own, wbo)], as_, ar, aps, apr)
        spread.start()
        spread.run()
        wait(keep)
        for layer in range(2):
            start(fetch(layer, layer))
    else:
        for layer in range(2):
            start(fetch(layer, layer))
        meet(at)

    def span(k):
        return pl.ds(pl.multiple_of(k * T, T), T)

    def moved(t, src, dst, send_sem, recv_sem):
        chip = at.across(t)
        return remote(src.at[span(chip), :], dst.at[span(t), :], send_sem.at[t], recv_sem.at[t], at.device(chip, at.core))

    def exchange(src, dst, send_sem, recv_sem):
        each(1, CHIPS, lambda t: moved(t, src, dst, send_sem, recv_sem).start())
        dst[pl.ds(0, T), :] = src[span(me), :]

    def weights(slot, cols):
        if perturbed:
            return bi[slot, :, cols], bo[slot, cols, :]
        return si[slot, :, cols].astype(bf16), so[slot, cols, :].astype(bf16)

    def kept(layer):
        return us.at[span(layer % KEPT), :]

    def put(layer):
        return pltpu.make_async_copy(kept(layer), u_hbm.at[layer], usem.at[layer % KEPT])

    def get(layer):
        return pltpu.make_async_copy(u_hbm.at[layer], kept(layer), usem.at[layer % KEPT])

    acc_t = acc.at[pl.ds(0, T), :]

    def layer_forward(layer, carry):
        slot = layer % 2
        hidden = hs[span((layer + 1) // 2), :]
        pre_out = kept(layer)

        @pl.when(layer >= KEPT + 2)
        def _():
            put(layer - KEPT).wait()

        wait(fetch(layer, slot))
        for j in range(0, F, FT):
            cols = pl.ds(j, FT)
            a_w, b_w = weights(slot, cols)
            pre = dot(hidden, a_w).astype(bf16)
            pre_out[:, cols] = pre
            pre = pre.astype(f32)
            part = dot((pre * cdf(pre)).astype(bf16), b_w)
            if j == 0:
                acc_t[...] = part
            else:
                acc_t[...] += part

        @pl.when(jnp.logical_and(layer >= 2, layer < KEPT))
        def _():
            put(layer).start()

        @pl.when(layer < LAYERS - 2)
        def _():
            start(fetch(layer + 2, slot))

        hs[span((layer + 2) // 2), :] = (hidden.astype(f32) + acc_t[...]).astype(bf16)
        return carry

    hs[pl.ds(0, T), :] = x_ref[...]
    lax.fori_loop(0, LAYERS, layer_forward, 0)
    exchange(hs, hg, hsend, hrecv)

    def share(value):
        sbuf[mine] = jnp.broadcast_to(value, (8, 128))

    def shared(i):
        return remote(sbuf.at[mine], sbuf.at[mine], ssend.at[i], srecv.at[mine], at.peer(i))

    def share_start():
        each(1, LAYERS, lambda i: shared(i).start())

    def share_finish():
        each(1, LAYERS, lambda i: shared(i).wait_send())

        def gathered(i):
            @pl.when(i != mine)
            def _():
                remote(sbuf.at[i], sbuf.at[i], ssend.at[0], srecv.at[i], at.partner()).wait_recv()

        each(0, LAYERS, gathered)
        total = sbuf[0]
        for i in range(1, LAYERS):
            total = total + sbuf[i]
        return total

    resid = hs[pl.ds(CHIPS * T, T), :].astype(f32) - y_ref[...].astype(f32)
    ds[pl.ds((CHIPS - 1) * T, T), :] = (resid * inv_count).astype(bf16)
    if perturbed:
        share(0.5 * jnp.sum(resid * resid, axis=(0, 1), keepdims=True))

    def layer_backward(i, carry):
        layer = LAYERS - 1 - i
        slot = layer % 2
        cot = ds[span((layer - 1) // 2), :]
        pre_in = kept(layer)

        @pl.when(layer < KEPT)
        def _():
            get(layer).wait()

        @pl.when(layer < LAYERS - 2)
        def _():
            wait(fetch(layer, slot))

        for j in range(0, F, FT):
            cols = pl.ds(j, FT)
            a_w, b_w = weights(slot, cols)
            pre = pre_in[:, cols].astype(f32)
            err = (dot(cot, b_w, NT) * (cdf(pre) + slope_tail(pre))).astype(bf16)
            part = dot(err, a_w, NT)
            if j == 0:
                acc_t[...] = part
            else:
                acc_t[...] += part

        @pl.when(layer >= KEPT + 2)
        def _():
            get(layer - KEPT).start()

        @pl.when(layer >= 4)
        def _():
            start(fetch(layer - 2, slot))

        @pl.when(layer < 4)
        def _():
            start(fetch(me * 2 + 3 - layer, slot))

        ds[span((layer - 2) // 2), :] = (cot.astype(f32) + acc_t[...]).astype(bf16)
        return carry

    lax.fori_loop(0, LAYERS - 2, layer_backward, 0)
    exchange(ds, dg, dsend, drecv)
    if perturbed:
        share_start()
    low, high = 1, 0

    def take(layer, slot):
        wait(fetch(layer, slot))
        if not perturbed:
            for j in range(0, F, FT):
                cols = pl.ds(j, FT)
                bi[slot, :, cols], bo[slot, cols, :] = weights(slot, cols)

    def block(i):
        return pl.ds(pl.multiple_of(i * KB_ROWS, KB_ROWS), KB_ROWS)

    def arrive(i, src, dst, send_sem, recv_sem):
        def step(t):
            @pl.when(t * T // KB_ROWS == i)
            def _():
                moved(t, src, dst, send_sem, recv_sem).wait_recv()

        each(1, CHIPS, step)

    def add(i, ref, which, cols, value):
        ref[which, :, cols] = jnp.where(i == 0, 0.0, ref[which, :, cols]) + value

    def sweep_low(i, carry):
        arrive(i, hs, hg, hsend, hrecv)
        rows = block(i)
        h_low = hg[rows, :]
        acc[...] = h_low.astype(f32)
        for j in range(0, F, KB_FT):
            cols = pl.ds(j, KB_FT)
            pre = dot(h_low, bi[low, :, cols]).astype(bf16)
            us[rows, cols] = pre
            pre = pre.astype(f32)
            acc[...] += dot((pre * cdf(pre)).astype(bf16), bo[low, cols, :])
        hs[rows, :] = acc[...].astype(bf16)
        return carry

    def sweep_high(i, carry):
        arrive(i, ds, dg, dsend, drecv)
        rows = block(i)
        h_mid, d_top = hs[rows, :], dg[rows, :]
        h_mid_t, d_top_t = h_mid.T, d_top.T
        acc[...] = d_top.astype(f32)
        for j in range(0, F, KB_FT):
            cols = pl.ds(j, KB_FT)
            pre = dot(h_mid, bi[high, :, cols]).astype(bf16).astype(f32)
            half = cdf(pre)
            post = (pre * half).astype(bf16)
            err = (dot(d_top, bo[high, cols, :], NT) * (half + slope_tail(pre))).astype(bf16)
            add(i, go, 1, cols, dot(d_top_t, post))
            add(i, gi, 1, cols, dot(h_mid_t, err))
            acc[...] += dot(err, bi[high, :, cols], NT)
        dg[rows, :] = acc[...].astype(bf16)
        return carry

    def sweep_back(i, carry):
        if perturbed:
            @pl.when(jnp.logical_and(i == 1, at.core == 1))
            def _():
                update()

        rows = block(i)
        h_low, d_mid = hg[rows, :], dg[rows, :]
        h_low_t, d_mid_t = h_low.T, d_mid.T
        for j in range(0, F, KB_FT):
            cols = pl.ds(j, KB_FT)
            pre = us[rows, cols].astype(f32)
            half = cdf(pre)
            post = (pre * half).astype(bf16)
            err = (dot(d_mid, bo[low, cols, :], NT) * (half + slope_tail(pre))).astype(bf16)
            add(i, go, 0, cols, dot(d_mid_t, post))
            add(i, gi, 0, cols, dot(h_low_t, err))
        return carry

    def swap(which):
        return [remote(gi.at[which], ri, xsend.at[0], xrecv.at[0], at.partner()),
                remote(go.at[which], ro, xsend.at[1], xrecv.at[1], at.partner())]

    def squares(value, total):
        sq = value * value
        for r in range(0, sq.shape[0], 8):
            for q in range(0, sq.shape[1], 128):
                total = total + sq[r:r + 8, q:q + 128]
        return total

    R, C = 16, 128

    def sum_in(i, total):
        rows = pl.ds(pl.multiple_of(i * R, R), R)
        g = gi[at.core, rows, :] + ri[rows, :]
        if perturbed:
            wi[rows, :] = wi[rows, :] - LEARN_RATE * g
            return total
        ri[rows, :] = g
        return squares(g, total)

    def sum_out(i, total):
        cols = pl.ds(pl.multiple_of(i * C, C), C)
        g = go[at.core, :, cols] + ro[:, cols]
        if perturbed:
            wo[cols, :] = wo[cols, :] - LEARN_RATE * g.T
            return total
        ro[:, cols] = g
        return squares(g, total)

    def sum_layer():
        got = swap(0)
        got[0].wait_recv()
        total = lax.fori_loop(0, D // R, sum_in, jnp.zeros((8, 128), f32))
        got[1].wait_recv()
        return lax.fori_loop(0, F // C, sum_out, total)

    if perturbed:
        gather = Gather(at, [(wi, wi_out), (wo, wo_out)], gs, gr, gps, gpr)
        keep_new = [pltpu.make_async_copy(wi, wi_out.at[mine], wsem.at[0]), pltpu.make_async_copy(wo, wo_out.at[mine], wsem.at[1])]

    def update():
        wait(own_w)
        sum_layer()
        gather.start()
        start(keep_new)

    blocks = ROWS // KB_ROWS
    take(me * 2, low)
    each(1, CHIPS, lambda t: moved(t, hs, hg, hsend, hrecv).wait_send())
    lax.fori_loop(0, blocks, sweep_low, 0)
    take(me * 2 + 1, high)
    if not perturbed:
        start(own_w)
    lax.fori_loop(0, blocks, sweep_high, 0)

    @pl.when(at.core == 0)
    def _():
        start(swap(1))

    lax.fori_loop(0, blocks, sweep_back, 0)

    @pl.when(at.core == 1)
    def _():
        start(swap(0))

    each(1, CHIPS, lambda t: moved(t, ds, dg, dsend, drecv).wait_send())
    if perturbed:
        @pl.when(at.core == 0)
        def _():
            update()

        gather.run()
        loss_out[...] = share_finish() * inv_count
        spread.finish()
        gather.finish()
        wait(keep_new)
    else:
        wait(own_w)
        sbuf[mine] = sum_layer()
        share_start()
        scale = radius / jnp.sqrt(jnp.sum(share_finish(), axis=(0, 1), keepdims=True))

        def perturb_in(i, carry):
            rows = pl.ds(pl.multiple_of(i * R, R), R)
            bi[0, rows, :] = (si[0, rows, :] + scale * ri[rows, :]).astype(bf16)
            return carry

        def perturb_out(i, carry):
            cols = pl.ds(pl.multiple_of(i * C, C), C)
            bo[0, cols, :] = (so[0, cols, :] + scale * ro[:, cols].T).astype(bf16)
            return carry

        lax.fori_loop(0, D // R, perturb_in, 0)
        lax.fori_loop(0, F // C, perturb_out, 0)
        done = [pltpu.make_async_copy(bi.at[0], wi_out, wsem.at[2]), pltpu.make_async_copy(bo.at[0], wo_out, wsem.at[3])]
        start(done)
        wait(done)
    for c in swap(0):
        c.wait_send()


def one_pass(perturbed, inv_count, radius, x, y, w_in, w_out, pert=()):
    acts = ((LAYERS, T, F), bf16)
    scratch = [
        pltpu.VMEM((2, D, F), bf16), pltpu.VMEM((2, F, D), bf16),
        pltpu.VMEM((ROWS + T, D), bf16), pltpu.VMEM((ROWS, D), bf16), pltpu.VMEM((KB_ROWS, D), f32), pltpu.VMEM((ROWS, F), bf16),
        pltpu.VMEM((ROWS, D), bf16), pltpu.VMEM((ROWS, D), bf16),
        pltpu.VMEM((2, D, F), f32), pltpu.VMEM((2, D, F), f32), pltpu.VMEM((D, F), f32), pltpu.VMEM((D, F), f32),
        DMA((CHIPS,)), DMA((CHIPS,)), DMA((CHIPS,)), DMA((CHIPS,)), DMA((KEPT,)), DMA((2, 2)), DMA((4,)), DMA((2,)), DMA((2,)),
        pltpu.VMEM((LAYERS, 8, 128), f32), DMA((LAYERS,)), DMA((LAYERS,)),
    ]
    if perturbed:
        shapes = [((LAYERS, D, F), f32), ((LAYERS, F, D), f32), ((LAYERS, D, F), bf16), ((LAYERS, F, D), bf16), acts, ((8, 128), f32)]
        out_specs = [ANY] * 5 + [V]
        scratch += [pltpu.VMEM((D, F), f32), pltpu.VMEM((F, D), f32), *GATHER_SEMS, *GATHER_SEMS]
    else:
        shapes = [((D, F), bf16), ((F, D), bf16), acts]
        out_specs = [ANY] * 3
        scratch += [pltpu.VMEM((2, D, F), f32), pltpu.VMEM((2, F, D), f32), DMA((2, 2))]
    options = dict(
        out_shape=[jax.ShapeDtypeStruct(*s) for s in shapes],
        in_specs=[V, V, ANY, ANY] + [V] * len(pert),
        out_specs=out_specs,
        scratch_shapes=scratch,
        compiler_params=pltpu.CompilerParams(
            collective_id=1 if perturbed else 0, has_side_effects=True, vmem_limit_bytes=VMEM_LIMIT),
        name="second_pass" if perturbed else "first_pass",
    )
    kernel = functools.partial(pass_kernel, perturbed, inv_count, radius)
    if perturbed:
        return pl.pallas_call(kernel, **options)(x, y, w_in, w_out, *pert)
    return pl.pallas_call(kernel, **options)(x, y, w_in, w_out)


def solution(mesh):
    mesh_axes = tuple(mesh.axis_names)
    dev_count = math.prod([mesh.shape[axis_name] for axis_name in mesh_axes])
    batch_spec = P(mesh_axes, None, None)

    def local_step(images, targets, w_in, w_out):
        layers, model_dim, hidden_dim = w_in.shape
        inv_count = 1.0 / (images.shape[0] * images.shape[1] * dev_count * model_dim)
        radius = RHO_REL * math.sqrt(layers * hidden_dim + model_dim)
        x, y = images.reshape(T, D), targets.reshape(T, D)
        pert = one_pass(False, inv_count, radius, x, y, w_in, w_out)[:2]
        new_in, new_out, _, _, _, loss = one_pass(True, inv_count, radius, x, y, w_in, w_out, pert)
        return new_in, new_out, loss[0, 0]

    return jax.shard_map(local_step, mesh=mesh, in_specs=(batch_spec, batch_spec, P(), P()), out_specs=(P(), P(), P()), check_vma=False)
```

```python
import functools
import math

import jax
import jax.numpy as jnp
from jax import lax
from jax.experimental import pallas as pl
from jax.experimental.pallas import tpu as pltpu
from jax.sharding import PartitionSpec as P

MESH = pl.DeviceIdType.MESH
RHO_REL = 0.1
LEARN_RATE = 8.0
SQRT_HALF = 0.7071067811865476
INV_SQRT_2PI = 0.3989422804014327
HALF_LOG2E = -0.7213475204444817

CHIPS = 8
LAYERS = 16
D = 384
F = 1536
T = 576
ROWS = CHIPS * T
FT = 768
KB_ROWS = 768
KB_FT = 256
KEPT = 8
PIECE = 144
VMEM_LIMIT = 67043328

f32, bf16 = jnp.float32, jnp.bfloat16
NN = (((1,), (0,)), ((), ()))
NT = (((1,), (1,)), ((), ()))
V = pl.BlockSpec(memory_space=pltpu.VMEM)
ANY = pl.BlockSpec(memory_space=pl.ANY)
DMA = pltpu.SemaphoreType.DMA


def dot(a, b, dims=NN):
    return lax.dot_general(a, b, dims, preferred_element_type=f32)


def cdf(x):
    return 0.5 * (1.0 + lax.erf(x * SQRT_HALF))


def slope_tail(x):
    return x * INV_SQRT_2PI * jnp.exp2((x * x) * HALF_LOG2E)


class Place:
    def __init__(self):
        self.z, self.y, data = lax.axis_index("model"), lax.axis_index("sub"), lax.axis_index("data")
        self.x, self.core = data // 2, data % 2
        self.chip = self.z * 4 + self.y * 2 + self.x
        self.mine = self.chip * 2 + self.core

    def across(self, t):
        x, y, z = (self.x + t) % 2, (self.y + t // 2) % 2, (self.z + t // 4) % 2
        return z * 4 + y * 2 + x

    def device(self, chip, core):
        return (chip // 4, (chip // 2) % 2, (chip % 2) * 2 + core)

    def partner(self):
        return self.device(self.chip, 1 - self.core)

    def peer(self, i):
        return self.device(self.across(i // 2), (self.core + i) % 2)


def bit(dim):
    return 1 + dim + dim * (dim - 1) // 2


def each(first, last, body):
    def step(i, carry):
        body(i)
        return carry

    lax.fori_loop(first, last, step, 0)


def meet(at):
    barrier = pltpu.get_barrier_semaphore()
    each(1, 16, lambda i: pl.semaphore_signal(barrier, inc=1, device_id=at.peer(i), device_id_type=MESH))
    pl.semaphore_wait(barrier, 15)


def remote(src, dst, send_sem, recv_sem, device):
    return pltpu.make_async_remote_copy(
        src_ref=src, dst_ref=dst, send_sem=send_sem, recv_sem=recv_sem, device_id=device, device_id_type=MESH
    )


class Gather:
    MESSAGES = ((0, ()), (1, ()), (2, ()), (1, (1,)), (2, (2,)), (2, (1,)), (2, (1, 2)))

    def __init__(self, at, tensors, send, recv, pair_send, pair_recv):
        self.at, self.tensors = at, tensors
        self.sems = (send, recv, pair_send, pair_recv)

    def make(self, i, part, own, chip, send, recv, device):
        ref, slots = self.tensors[i]
        n = slots.shape[1] // 3
        rows = pl.ds(pl.multiple_of(part * n, n), n)
        dst = slots.at[chip * 2 + self.at.core, rows, :]
        return remote(ref.at[rows, :] if own else dst, dst, send, recv, device)

    def parts(self, dim, slot):
        back, turns = self.MESSAGES[slot]
        t = 0
        for o in turns:
            t = t + bit((dim + 3 - o) % 3)
        return (dim + 3 - back) % 3, t

    def link(self, i, dim, slot):
        part, t = self.parts(dim, slot)
        send, recv, _, _ = self.sems
        return self.make(i, part, slot < 3, self.at.across(t) if slot >= 3 else self.at.chip, send.at[dim, slot, i],
                         recv.at[dim, slot, i], self.at.device(self.at.across(bit(dim)), self.at.core))

    def pair(self, i, part, own, chip, index):
        _, _, send, recv = self.sems
        return self.make(i, part, own, chip, send.at[index, i], recv.at[index, i], self.at.partner())

    def start(self):
        for slot in range(3):
            for i in range(2):
                each(0, 3, lambda dim: self.link(i, dim, slot).start())
        for i in range(2):
            each(0, 3, lambda part: self.pair(i, part, True, self.at.chip, part).start())

    def run(self):
        turn = {0: (3, 1), 1: (5, 1), 3: (6, 1)}
        for slot in range(7):
            for i in range(2):
                def got(dim):
                    self.link(i, dim, slot).wait_recv()
                    if slot in turn:
                        later, step = turn[slot]
                        self.link(i, (dim + step) % 3, later).start()
                    part, t = self.parts(dim, slot)
                    self.pair(i, part, False, self.at.across(t + bit(dim)), 3 + slot * 3 + dim).start()

                each(0, 3, got)
            if slot == 0:
                for i in range(2):
                    each(0, 3, lambda dim: self.link(i, dim, 4).start())
        for i in range(2):
            each(0, 24, lambda index: self.pair(i, 0, False, self.at.chip, index).wait_recv())

    def finish(self):
        for i in range(2):
            each(0, 24, lambda index: self.pair(i, 0, False, self.at.chip, index).wait_send())
            for slot in range(7):
                each(0, 3, lambda dim: self.link(i, dim, slot).wait_send())


GATHER_SEMS = [DMA((3, 7, 2)), DMA((3, 7, 2)), DMA((24, 2)), DMA((24, 2))]


def pass_kernel(perturbed, inv_count, radius, *refs):
    if perturbed:
        (x_ref, y_ref, wi_hbm, wo_hbm, pi_own, po_own, wi_out, wo_out, wbi, wbo, u_hbm, loss_out,
         bi, bo, hs, ds, hm, us, hg, dg, gi, go, ri, ro,
         hsend, hrecv, dsend, drecv, usem, bsem, wsem, xsend, xrecv, sbuf, ssend, srecv,
         wi, wo, as_, ar, aps, apr, gs, gr, gps, gpr) = refs
    else:
        (x_ref, y_ref, wi_hbm, wo_hbm, wi_out, wo_out, u_hbm,
         bi, bo, hs, ds, hm, us, hg, dg, gi, go, ri, ro,
         hsend, hrecv, dsend, drecv, usem, bsem, wsem, xsend, xrecv, sbuf, ssend, srecv,
         si, so, fsem) = refs
    at = Place()
    me = at.chip
    mine = at.mine

    def fetch32(layer, slot):
        return (pltpu.make_async_copy(wi_hbm.at[layer], si.at[slot], fsem.at[slot, 0]),
                pltpu.make_async_copy(wo_hbm.at[layer], so.at[slot], fsem.at[slot, 1]))

    def fetch16(layer, slot):
        return (pltpu.make_async_copy(wbi.at[layer], bi.at[slot], bsem.at[slot, 0]),
                pltpu.make_async_copy(wbo.at[layer], bo.at[slot], bsem.at[slot, 1]))

    fetch = fetch16 if perturbed else fetch32

    def start(copies):
        for c in copies:
            c.start()

    def wait(copies):
        for c in copies:
            c.wait()

    own_w = [pltpu.make_async_copy(wi_hbm.at[mine], wi if perturbed else si.at[0], wsem.at[0]),
             pltpu.make_async_copy(wo_hbm.at[mine], wo if perturbed else so.at[0], wsem.at[1])]
    if perturbed:
        keep = [pltpu.make_async_copy(pi_own, wbi.at[mine], wsem.at[2]), pltpu.make_async_copy(po_own, wbo.at[mine], wsem.at[3])]
        start(keep)
        start(own_w)
        meet(at)
        spread = Gather(at, [(pi_own, wbi), (po_own, wbo)], as_, ar, aps, apr)
        spread.start()
        spread.run()
        wait(keep)
        for layer in range(2):
            start(fetch(layer, layer))
    else:
        for layer in range(2):
            start(fetch(layer, layer))
        meet(at)

    def span(k):
        return pl.ds(pl.multiple_of(k * T, T), T)

    def moved(t, src, dst, send_sem, recv_sem):
        chip = at.across(t)
        return remote(src.at[span(chip), :], dst.at[span(t), :], send_sem.at[t], recv_sem.at[t], at.device(chip, at.core))

    def exchange(src, dst, send_sem, recv_sem):
        for group in ((1, 2, 4), (3, 5, 6), (7,)):
            def step(q):
                for t in group:
                    chip = at.across(t)
                    remote(src.at[pl.ds(pl.multiple_of(chip * T + q * PIECE, 16), PIECE), :],
                           dst.at[pl.ds(pl.multiple_of(t * T + q * PIECE, 16), PIECE), :],
                           send_sem.at[t], recv_sem.at[t], at.device(chip, at.core)).start()

            each(0, T // PIECE, step)
        dst[pl.ds(0, T), :] = src[span(me), :]

    def weights(slot, cols):
        if perturbed:
            return bi[slot, :, cols], bo[slot, cols, :]
        return si[slot, :, cols].astype(bf16), so[slot, cols, :].astype(bf16)

    def kept(layer):
        return us.at[span(layer % KEPT), :]

    def put(layer):
        return pltpu.make_async_copy(kept(layer), u_hbm.at[layer], usem.at[layer % KEPT])

    def get(layer):
        return pltpu.make_async_copy(u_hbm.at[layer], kept(layer), usem.at[layer % KEPT])

    def layer_forward(layer, carry):
        slot = layer % 2
        hidden = hs[span((layer + 1) // 2), :]
        pre_out = kept(layer)

        @pl.when(layer >= KEPT + 2)
        def _():
            put(layer - KEPT).wait()

        wait(fetch(layer, slot))
        total = hidden.astype(f32)
        for j in range(0, F, FT):
            cols = pl.ds(j, FT)
            a_w, b_w = weights(slot, cols)
            pre = dot(hidden, a_w).astype(bf16)
            pre_out[:, cols] = pre
            pre = pre.astype(f32)
            total = total + dot((pre * cdf(pre)).astype(bf16), b_w)

        @pl.when(jnp.logical_and(layer >= 2, layer < KEPT))
        def _():
            put(layer).start()

        @pl.when(layer < LAYERS - 2)
        def _():
            start(fetch(layer + 2, slot))

        hs[span((layer + 2) // 2), :] = total.astype(bf16)
        return carry

    hs[pl.ds(0, T), :] = x_ref[...]
    lax.fori_loop(0, LAYERS, layer_forward, 0)
    exchange(hs, hg, hsend, hrecv)

    def share(value):
        sbuf[mine] = jnp.broadcast_to(value, (8, 128))

    def shared(i):
        return remote(sbuf.at[mine], sbuf.at[mine], ssend.at[i], srecv.at[mine], at.peer(i))

    def share_start():
        each(1, LAYERS, lambda i: shared(i).start())

    def share_finish():
        each(1, LAYERS, lambda i: shared(i).wait_send())

        def gathered(i):
            @pl.when(i != mine)
            def _():
                remote(sbuf.at[i], sbuf.at[i], ssend.at[0], srecv.at[i], at.partner()).wait_recv()

        each(0, LAYERS, gathered)
        total = sbuf[0]
        for i in range(1, LAYERS):
            total = total + sbuf[i]
        return total

    resid = hs[pl.ds(CHIPS * T, T), :].astype(f32) - y_ref[...].astype(f32)
    ds[pl.ds((CHIPS - 1) * T, T), :] = (resid * inv_count).astype(bf16)
    if perturbed:
        share(0.5 * jnp.sum(resid * resid, axis=(0, 1), keepdims=True))

    def layer_backward(i, carry):
        layer = LAYERS - 1 - i
        slot = layer % 2
        cot = ds[span((layer - 1) // 2), :]
        pre_in = kept(layer)

        @pl.when(layer < KEPT)
        def _():
            get(layer).wait()

        @pl.when(layer < LAYERS - 2)
        def _():
            wait(fetch(layer, slot))

        total = cot.astype(f32)
        for j in range(0, F, FT):
            cols = pl.ds(j, FT)
            a_w, b_w = weights(slot, cols)
            pre = pre_in[:, cols].astype(f32)
            err = (dot(cot, b_w, NT) * (cdf(pre) + slope_tail(pre))).astype(bf16)
            total = total + dot(err, a_w, NT)

        @pl.when(layer >= KEPT + 2)
        def _():
            get(layer - KEPT).start()

        @pl.when(layer >= 4)
        def _():
            start(fetch(layer - 2, slot))

        @pl.when(layer < 4)
        def _():
            start(fetch(me * 2 + 3 - layer, slot))

        ds[span((layer - 2) // 2), :] = total.astype(bf16)
        return carry

    lax.fori_loop(0, LAYERS - 2, layer_backward, 0)
    exchange(ds, dg, dsend, drecv)
    if perturbed:
        share_start()
    low, high = 1, 0

    def take(layer, slot):
        wait(fetch(layer, slot))
        if not perturbed:
            for j in range(0, F, FT):
                cols = pl.ds(j, FT)
                bi[slot, :, cols], bo[slot, cols, :] = weights(slot, cols)

    def block(i):
        return pl.ds(pl.multiple_of(i * KB_ROWS, KB_ROWS), KB_ROWS)

    def arrive(i, src, dst, send_sem, recv_sem):
        def step(t):
            @pl.when(t * T // KB_ROWS == i)
            def _():
                moved(t, src, dst, send_sem, recv_sem).wait_recv()

        each(1, CHIPS, step)

    def add(i, ref, which, cols, value):
        ref[which, :, cols] = jnp.where(i == 0, 0.0, ref[which, :, cols]) + value

    def sweep_low(i, carry):
        arrive(i, hs, hg, hsend, hrecv)
        rows = block(i)
        h_low = hg[rows, :]
        total = h_low.astype(f32)
        for j in range(0, F, FT):
            cols = pl.ds(j, FT)
            pre = dot(h_low, bi[low, :, cols]).astype(bf16)
            us[rows, cols] = pre
            pre = pre.astype(f32)
            total = total + dot((pre * cdf(pre)).astype(bf16), bo[low, cols, :])
        hm[rows, :] = total.astype(bf16)
        return carry

    def sweep_high(i, carry):
        arrive(i, ds, dg, dsend, drecv)
        rows = block(i)
        h_mid, d_top = hm[rows, :], dg[rows, :]
        h_mid_t, d_top_t = h_mid.T, d_top.T
        total = d_top.astype(f32)
        for j in range(0, F, KB_FT):
            cols = pl.ds(j, KB_FT)
            pre = dot(h_mid, bi[high, :, cols]).astype(bf16).astype(f32)
            half = cdf(pre)
            post = (pre * half).astype(bf16)
            err = (dot(d_top, bo[high, cols, :], NT) * (half + slope_tail(pre))).astype(bf16)
            add(i, go, 1, cols, dot(d_top_t, post))
            add(i, gi, 1, cols, dot(h_mid_t, err))
            total = total + dot(err, bi[high, :, cols], NT)
        dg[rows, :] = total.astype(bf16)
        return carry

    def sweep_back(i, carry):
        if perturbed:
            @pl.when(jnp.logical_and(i == 1, at.core == 1))
            def _():
                update()

        rows = block(i)
        h_low, d_mid = hg[rows, :], dg[rows, :]
        h_low_t, d_mid_t = h_low.T, d_mid.T
        for j in range(0, F, KB_FT):
            cols = pl.ds(j, KB_FT)
            pre = us[rows, cols].astype(f32)
            half = cdf(pre)
            post = (pre * half).astype(bf16)
            err = (dot(d_mid, bo[low, cols, :], NT) * (half + slope_tail(pre))).astype(bf16)
            add(i, go, 0, cols, dot(d_mid_t, post))
            add(i, gi, 0, cols, dot(h_low_t, err))
        return carry

    def swap(which):
        return [remote(gi.at[which], ri, xsend.at[0], xrecv.at[0], at.partner()),
                remote(go.at[which], ro, xsend.at[1], xrecv.at[1], at.partner())]

    def squares(value, total):
        sq = value * value
        for r in range(0, sq.shape[0], 8):
            for q in range(0, sq.shape[1], 128):
                total = total + sq[r:r + 8, q:q + 128]
        return total

    R, C = 16, 128

    def sum_in(i, total):
        rows = pl.ds(pl.multiple_of(i * R, R), R)
        g = gi[at.core, rows, :] + ri[rows, :]
        if perturbed:
            wi[rows, :] = wi[rows, :] - LEARN_RATE * g
            return total
        ri[rows, :] = g
        return squares(g, total)

    def sum_out(i, total):
        cols = pl.ds(pl.multiple_of(i * C, C), C)
        g = go[at.core, :, cols] + ro[:, cols]
        if perturbed:
            wo[cols, :] = wo[cols, :] - LEARN_RATE * g.T
            return total
        ro[:, cols] = g
        return squares(g, total)

    def sum_layer():
        got = swap(0)
        got[0].wait_recv()
        total = lax.fori_loop(0, D // R, sum_in, jnp.zeros((8, 128), f32))
        got[1].wait_recv()
        return lax.fori_loop(0, F // C, sum_out, total)

    if perturbed:
        gather = Gather(at, [(wi, wi_out), (wo, wo_out)], gs, gr, gps, gpr)
        keep_new = [pltpu.make_async_copy(wi, wi_out.at[mine], wsem.at[0]), pltpu.make_async_copy(wo, wo_out.at[mine], wsem.at[1])]

    def update():
        wait(own_w)
        sum_layer()
        gather.start()
        start(keep_new)

    blocks = ROWS // KB_ROWS
    take(me * 2, low)
    lax.fori_loop(0, blocks, sweep_low, 0)
    take(me * 2 + 1, high)
    if not perturbed:
        start(own_w)
    lax.fori_loop(0, blocks, sweep_high, 0)

    @pl.when(at.core == 0)
    def _():
        start(swap(1))

    lax.fori_loop(0, blocks, sweep_back, 0)

    @pl.when(at.core == 1)
    def _():
        start(swap(0))

    def sent(t):
        moved(t, hs, hg, hsend, hrecv).wait_send()
        moved(t, ds, dg, dsend, drecv).wait_send()

    each(1, CHIPS, sent)
    if perturbed:
        @pl.when(at.core == 0)
        def _():
            update()

        gather.run()
        loss_out[...] = share_finish() * inv_count
        spread.finish()
        gather.finish()
        wait(keep_new)
    else:
        wait(own_w)
        sbuf[mine] = sum_layer()
        share_start()
        scale = radius / jnp.sqrt(jnp.sum(share_finish(), axis=(0, 1), keepdims=True))

        def perturb_in(i, carry):
            rows = pl.ds(pl.multiple_of(i * R, R), R)
            bi[0, rows, :] = (si[0, rows, :] + scale * ri[rows, :]).astype(bf16)
            return carry

        def perturb_out(i, carry):
            cols = pl.ds(pl.multiple_of(i * C, C), C)
            bo[0, cols, :] = (so[0, cols, :] + scale * ro[:, cols].T).astype(bf16)
            return carry

        lax.fori_loop(0, D // R, perturb_in, 0)
        lax.fori_loop(0, F // C, perturb_out, 0)
        done = [pltpu.make_async_copy(bi.at[0], wi_out, wsem.at[2]), pltpu.make_async_copy(bo.at[0], wo_out, wsem.at[3])]
        start(done)
        wait(done)
    for c in swap(0):
        c.wait_send()


def one_pass(perturbed, inv_count, radius, x, y, w_in, w_out, pert=()):
    acts = ((LAYERS, T, F), bf16)
    scratch = [
        pltpu.VMEM((2, D, F), bf16), pltpu.VMEM((2, F, D), bf16),
        pltpu.VMEM((ROWS + T, D), bf16), pltpu.VMEM((ROWS, D), bf16), pltpu.VMEM((ROWS, D), bf16), pltpu.VMEM((ROWS, F), bf16),
        pltpu.VMEM((ROWS, D), bf16), pltpu.VMEM((ROWS, D), bf16),
        pltpu.VMEM((2, D, F), f32), pltpu.VMEM((2, D, F), f32), pltpu.VMEM((D, F), f32), pltpu.VMEM((D, F), f32),
        DMA((CHIPS,)), DMA((CHIPS,)), DMA((CHIPS,)), DMA((CHIPS,)), DMA((KEPT,)), DMA((2, 2)), DMA((4,)), DMA((2,)), DMA((2,)),
        pltpu.VMEM((LAYERS, 8, 128), f32), DMA((LAYERS,)), DMA((LAYERS,)),
    ]
    if perturbed:
        shapes = [((LAYERS, D, F), f32), ((LAYERS, F, D), f32), ((LAYERS, D, F), bf16), ((LAYERS, F, D), bf16), acts, ((8, 128), f32)]
        out_specs = [ANY] * 5 + [V]
        scratch += [pltpu.VMEM((D, F), f32), pltpu.VMEM((F, D), f32), *GATHER_SEMS, *GATHER_SEMS]
    else:
        shapes = [((D, F), bf16), ((F, D), bf16), acts]
        out_specs = [ANY] * 3
        scratch += [pltpu.VMEM((2, D, F), f32), pltpu.VMEM((2, F, D), f32), DMA((2, 2))]
    options = dict(
        out_shape=[jax.ShapeDtypeStruct(*s) for s in shapes],
        in_specs=[V, V, ANY, ANY] + [V] * len(pert),
        out_specs=out_specs,
        scratch_shapes=scratch,
        compiler_params=pltpu.CompilerParams(
            collective_id=1 if perturbed else 0, has_side_effects=True, vmem_limit_bytes=VMEM_LIMIT),
        name="second_pass" if perturbed else "first_pass",
    )
    kernel = functools.partial(pass_kernel, perturbed, inv_count, radius)
    if perturbed:
        return pl.pallas_call(kernel, **options)(x, y, w_in, w_out, *pert)
    return pl.pallas_call(kernel, **options)(x, y, w_in, w_out)


def solution(mesh):
    mesh_axes = tuple(mesh.axis_names)
    dev_count = math.prod([mesh.shape[axis_name] for axis_name in mesh_axes])
    batch_spec = P(mesh_axes, None, None)

    def local_step(images, targets, w_in, w_out):
        layers, model_dim, hidden_dim = w_in.shape
        inv_count = 1.0 / (images.shape[0] * images.shape[1] * dev_count * model_dim)
        radius = RHO_REL * math.sqrt(layers * hidden_dim + model_dim)
        x, y = images.reshape(T, D), targets.reshape(T, D)
        pert = one_pass(False, inv_count, radius, x, y, w_in, w_out)[:2]
        new_in, new_out, _, _, _, loss = one_pass(True, inv_count, radius, x, y, w_in, w_out, pert)
        return new_in, new_out, loss[0, 0]

    return jax.shard_map(local_step, mesh=mesh, in_specs=(batch_spec, batch_spec, P(), P()), out_specs=(P(), P(), P()), check_vma=False)
```

```python
import functools
import math

import jax
import jax.numpy as jnp
from jax import lax
from jax.experimental import pallas as pl
from jax.experimental.pallas import tpu as pltpu
from jax.sharding import PartitionSpec as P

MESH = pl.DeviceIdType.MESH
RHO_REL = 0.1
LEARN_RATE = 8.0
SQRT_HALF = 0.7071067811865476
INV_SQRT_2PI = 0.3989422804014327
HALF_LOG2E = -0.7213475204444817

CHIPS = 8
LAYERS = 16
D = 384
F = 1536
T = 576
ROWS = CHIPS * T
FT = 768
KB_ROWS = 768
KB_FT = 256
KEPT = 8
PIECE = 144
VMEM_LIMIT = 67043328

f32, bf16 = jnp.float32, jnp.bfloat16
NN = (((1,), (0,)), ((), ()))
NT = (((1,), (1,)), ((), ()))
V = pl.BlockSpec(memory_space=pltpu.VMEM)
ANY = pl.BlockSpec(memory_space=pl.ANY)
DMA = pltpu.SemaphoreType.DMA


def dot(a, b, dims=NN):
    return lax.dot_general(a, b, dims, preferred_element_type=f32)


def cdf(x):
    return 0.5 * (1.0 + lax.erf(x * SQRT_HALF))


def slope_tail(x):
    return x * INV_SQRT_2PI * jnp.exp2((x * x) * HALF_LOG2E)


def div(a, b):
    return lax.div(jnp.int32(a), jnp.int32(b))


def rem(a, b):
    return lax.rem(jnp.int32(a), jnp.int32(b))


def some(k):
    return div(k * k + 35, 36)


def bit(dim):
    return 1 + dim + div(dim * (dim - 1), 2)


class Place:
    def __init__(self):
        self.z, self.y, data = lax.axis_index("model"), lax.axis_index("sub"), lax.axis_index("data")
        self.x, self.core = div(data, 2), rem(data, 2)
        self.chip = self.z * 4 + self.y * 2 + self.x
        self.mine = self.chip * 2 + self.core

    def across(self, t):
        x, y, z = rem(self.x + t, 2), rem(self.y + div(t, 2), 2), rem(self.z + div(t, 4), 2)
        return z * 4 + y * 2 + x

    def device(self, chip, core):
        return (div(chip, 4), rem(div(chip, 2), 2), rem(chip, 2) * 2 + core)

    def partner(self):
        return self.device(self.chip, 1 - self.core)

    def peer(self, i):
        return self.device(self.across(div(i, 2)), rem(self.core + i, 2))


def each(first, last, body):
    def step(i, carry):
        body(i)
        return carry

    lax.fori_loop(first, last, step, 0)


def meet(at):
    barrier = pltpu.get_barrier_semaphore()
    each(1, 16, lambda i: pl.semaphore_signal(barrier, inc=1, device_id=at.peer(i), device_id_type=MESH))
    pl.semaphore_wait(barrier, 15)


def remote(src, dst, send_sem, recv_sem, device):
    return pltpu.make_async_remote_copy(
        src_ref=src, dst_ref=dst, send_sem=send_sem, recv_sem=recv_sem, device_id=device, device_id_type=MESH
    )


class Gather:
    def __init__(self, at, tensors, send, recv, pair_send, pair_recv):
        self.at, self.tensors = at, tensors
        self.sems = (send, recv, pair_send, pair_recv)

    def make(self, i, part, own, chip, send, recv, device):
        ref, slots = self.tensors[i]
        n = slots.shape[1] // 3
        rows = pl.ds(pl.multiple_of(part * n, n), n)
        dst = slots.at[chip * 2 + self.at.core, rows, :]
        return remote(ref.at[rows, :] if own else dst, dst, send, recv, device)

    def parts(self, dim, slot):
        later = some(slot) * some(slot - 1) * some(slot - 2)
        back = some(slot) + some(slot) * some(slot - 1) - 1 + some(slot - 3)
        one, two = later * some(slot - 4), later * (1 - rem(slot, 2))
        return rem(dim + 3 - back, 3), one * bit(rem(dim + 2, 3)) + two * bit(rem(dim + 1, 3))

    def link(self, i, dim, slot, own=False):
        part, t = (rem(dim + 3 - slot, 3), 0) if own else self.parts(dim, slot)
        send, recv, _, _ = self.sems
        index = slot * 3 + dim
        return self.make(i, part, own, self.at.chip if own else self.at.across(t), send.at[index, i], recv.at[index, i],
                         self.at.device(self.at.across(bit(dim)), self.at.core))

    def pair(self, i, part, own, chip, index):
        _, _, send, recv = self.sems
        return self.make(i, part, own, chip, send.at[index, i], recv.at[index, i], self.at.partner())

    def passing(self, i, index, which):
        return self.make(i, 0, False, self.at.chip, self.sems[which].at[index, i], self.sems[which + 1].at[index, i], self.at.partner())

    def start(self):
        def own(slot):
            for i in range(2):
                each(0, 3, lambda dim: self.link(i, dim, slot, own=True).start())

        each(0, 3, own)
        for i in range(2):
            each(0, 3, lambda part: self.pair(i, part, True, self.at.chip, part).start())

    def run(self):
        def step(slot):
            for i in range(2):
                def got(dim):
                    self.passing(i, slot * 3 + dim, 0).wait_recv()

                    @pl.when(jnp.logical_or(slot <= 1, slot == 3))
                    def _():
                        self.link(i, rem(dim + 1, 3), 3 + 2 * some(slot) + div(slot, 3)).start()

                    part, t = self.parts(dim, slot)
                    self.pair(i, part, False, self.at.across(t + bit(dim)), 3 + slot * 3 + dim).start()

                each(0, 3, got)

            @pl.when(slot == 0)
            def _():
                for i in range(2):
                    each(0, 3, lambda dim: self.link(i, dim, 4).start())

        each(0, 7, step)
        for i in range(2):
            each(0, 24, lambda index: self.passing(i, index, 2).wait_recv())

    def finish(self):
        for i in range(2):
            each(0, 24, lambda index: self.passing(i, index, 2).wait_send())
            each(0, 21, lambda index: self.passing(i, index, 0).wait_send())


GATHER_SEMS = [DMA((21, 2)), DMA((21, 2)), DMA((24, 2)), DMA((24, 2))]


def pass_kernel(perturbed, inv_count, radius, *refs):
    if perturbed:
        (x_ref, y_ref, wi_hbm, wo_hbm, pi_own, po_own, wi_out, wo_out, wbi, wbo, u_hbm, loss_out,
         bi, bo, hs, ds, hm, us, hg, dg, gi, go, ri, ro,
         hsend, hrecv, dsend, drecv, usem, bsem, wsem, xsend, xrecv, sbuf, ssend, srecv,
         wi, wo, as_, ar, aps, apr, gs, gr, gps, gpr) = refs
    else:
        (x_ref, y_ref, wi_hbm, wo_hbm, wi_out, wo_out, u_hbm,
         bi, bo, hs, ds, hm, us, hg, dg, gi, go, ri, ro,
         hsend, hrecv, dsend, drecv, usem, bsem, wsem, xsend, xrecv, sbuf, ssend, srecv,
         si, so, fsem) = refs
    at = Place()
    me = at.chip
    mine = at.mine

    def fetch32(layer, slot):
        return (pltpu.make_async_copy(wi_hbm.at[layer], si.at[slot], fsem.at[slot, 0]),
                pltpu.make_async_copy(wo_hbm.at[layer], so.at[slot], fsem.at[slot, 1]))

    def fetch16(layer, slot):
        return (pltpu.make_async_copy(wbi.at[layer], bi.at[slot], bsem.at[slot, 0]),
                pltpu.make_async_copy(wbo.at[layer], bo.at[slot], bsem.at[slot, 1]))

    fetch = fetch16 if perturbed else fetch32

    def start(copies):
        for c in copies:
            c.start()

    def wait(copies):
        for c in copies:
            c.wait()

    own_w = [pltpu.make_async_copy(wi_hbm.at[mine], wi if perturbed else si.at[0], wsem.at[0]),
             pltpu.make_async_copy(wo_hbm.at[mine], wo if perturbed else so.at[0], wsem.at[1])]
    if perturbed:
        keep = [pltpu.make_async_copy(pi_own, wbi.at[mine], wsem.at[2]), pltpu.make_async_copy(po_own, wbo.at[mine], wsem.at[3])]
        start(keep)
        start(own_w)
        meet(at)
        spread = Gather(at, [(pi_own, wbi), (po_own, wbo)], as_, ar, aps, apr)
        spread.start()
        spread.run()
        wait(keep)
        for layer in range(2):
            start(fetch(layer, layer))
    else:
        for layer in range(2):
            start(fetch(layer, layer))
        meet(at)

    def span(k):
        return pl.ds(pl.multiple_of(k * T, T), T)

    def moved(t, src, dst, send_sem, recv_sem):
        chip = at.across(t)
        return remote(src.at[span(chip), :], dst.at[span(t), :], send_sem.at[t], recv_sem.at[t], at.device(chip, at.core))

    def exchange(src, dst, send_sem, recv_sem):
        for group in ((1, 2, 4), (3, 5, 6), (7,)):
            def step(q):
                for t in group:
                    chip = at.across(t)
                    remote(src.at[pl.ds(pl.multiple_of(chip * T + q * PIECE, 16), PIECE), :],
                           dst.at[pl.ds(pl.multiple_of(t * T + q * PIECE, 16), PIECE), :],
                           send_sem.at[t], recv_sem.at[t], at.device(chip, at.core)).start()

            each(0, T // PIECE, step)
        dst[pl.ds(0, T), :] = src[span(me), :]

    def weights(slot, cols):
        if perturbed:
            return bi[slot, :, cols], bo[slot, cols, :]
        return si[slot, :, cols].astype(bf16), so[slot, cols, :].astype(bf16)

    def kept(layer):
        return us.at[span(layer % KEPT), :]

    def put(layer):
        return pltpu.make_async_copy(kept(layer), u_hbm.at[layer], usem.at[layer % KEPT])

    def get(layer):
        return pltpu.make_async_copy(u_hbm.at[layer], kept(layer), usem.at[layer % KEPT])

    def layer_forward(layer, carry):
        slot = layer % 2
        hidden = hs[span((layer + 1) // 2), :]
        pre_out = kept(layer)

        @pl.when(layer >= KEPT + 2)
        def _():
            put(layer - KEPT).wait()

        wait(fetch(layer, slot))
        total = hidden.astype(f32)
        for j in range(0, F, FT):
            cols = pl.ds(j, FT)
            a_w, b_w = weights(slot, cols)
            pre = dot(hidden, a_w).astype(bf16)
            pre_out[:, cols] = pre
            pre = pre.astype(f32)
            total = total + dot((pre * cdf(pre)).astype(bf16), b_w)

        @pl.when(jnp.logical_and(layer >= 2, layer < KEPT))
        def _():
            put(layer).start()

        @pl.when(layer < LAYERS - 2)
        def _():
            start(fetch(layer + 2, slot))

        hs[span((layer + 2) // 2), :] = total.astype(bf16)
        return carry

    hs[pl.ds(0, T), :] = x_ref[...]
    lax.fori_loop(0, LAYERS, layer_forward, 0)
    exchange(hs, hg, hsend, hrecv)

    def share(value):
        sbuf[mine] = jnp.broadcast_to(value, (8, 128))

    def shared(i):
        return remote(sbuf.at[mine], sbuf.at[mine], ssend.at[i], srecv.at[mine], at.peer(i))

    def share_start():
        each(1, LAYERS, lambda i: shared(i).start())

    def share_finish():
        each(1, LAYERS, lambda i: shared(i).wait_send())

        def gathered(i):
            @pl.when(i != mine)
            def _():
                remote(sbuf.at[i], sbuf.at[i], ssend.at[0], srecv.at[i], at.partner()).wait_recv()

        each(0, LAYERS, gathered)
        total = sbuf[0]
        for i in range(1, LAYERS):
            total = total + sbuf[i]
        return total

    resid = hs[pl.ds(CHIPS * T, T), :].astype(f32) - y_ref[...].astype(f32)
    ds[pl.ds((CHIPS - 1) * T, T), :] = (resid * inv_count).astype(bf16)
    if perturbed:
        share(0.5 * jnp.sum(resid * resid, axis=(0, 1), keepdims=True))

    def layer_backward(i, carry):
        layer = LAYERS - 1 - i
        slot = layer % 2
        cot = ds[span((layer - 1) // 2), :]
        pre_in = kept(layer)

        @pl.when(layer < KEPT)
        def _():
            get(layer).wait()

        @pl.when(layer < LAYERS - 2)
        def _():
            wait(fetch(layer, slot))

        total = cot.astype(f32)
        for j in range(0, F, FT):
            cols = pl.ds(j, FT)
            a_w, b_w = weights(slot, cols)
            pre = pre_in[:, cols].astype(f32)
            err = (dot(cot, b_w, NT) * (cdf(pre) + slope_tail(pre))).astype(bf16)
            total = total + dot(err, a_w, NT)

        @pl.when(layer >= KEPT + 2)
        def _():
            get(layer - KEPT).start()

        @pl.when(layer >= 4)
        def _():
            start(fetch(layer - 2, slot))

        @pl.when(layer < 4)
        def _():
            start(fetch(me * 2 + 3 - layer, slot))

        ds[span((layer - 2) // 2), :] = total.astype(bf16)
        return carry

    lax.fori_loop(0, LAYERS - 2, layer_backward, 0)
    exchange(ds, dg, dsend, drecv)
    if perturbed:
        share_start()
    low, high = 1, 0

    def take(layer, slot):
        wait(fetch(layer, slot))
        if not perturbed:
            for j in range(0, F, FT):
                cols = pl.ds(j, FT)
                bi[slot, :, cols], bo[slot, cols, :] = weights(slot, cols)

    def block(i):
        return pl.ds(pl.multiple_of(i * KB_ROWS, KB_ROWS), KB_ROWS)

    def arrive(i, src, dst, send_sem, recv_sem):
        def step(t):
            @pl.when(t * T // KB_ROWS == i)
            def _():
                moved(t, src, dst, send_sem, recv_sem).wait_recv()

        each(1, CHIPS, step)

    def add(i, ref, which, cols, value):
        ref[which, :, cols] = jnp.where(i == 0, 0.0, ref[which, :, cols]) + value

    def sweep_low(i, carry):
        arrive(i, hs, hg, hsend, hrecv)
        rows = block(i)
        h_low = hg[rows, :]
        total = h_low.astype(f32)
        for j in range(0, F, FT):
            cols = pl.ds(j, FT)
            pre = dot(h_low, bi[low, :, cols]).astype(bf16)
            us[rows, cols] = pre
            pre = pre.astype(f32)
            total = total + dot((pre * cdf(pre)).astype(bf16), bo[low, cols, :])
        hm[rows, :] = total.astype(bf16)
        return carry

    def sweep_high(i, carry):
        arrive(i, ds, dg, dsend, drecv)
        rows = block(i)
        h_mid, d_top = hm[rows, :], dg[rows, :]
        h_mid_t, d_top_t = h_mid.T, d_top.T
        total = d_top.astype(f32)
        for j in range(0, F, KB_FT):
            cols = pl.ds(j, KB_FT)
            pre = dot(h_mid, bi[high, :, cols]).astype(bf16).astype(f32)
            half = cdf(pre)
            post = (pre * half).astype(bf16)
            err = (dot(d_top, bo[high, cols, :], NT) * (half + slope_tail(pre))).astype(bf16)
            add(i, go, 1, cols, dot(d_top_t, post))
            add(i, gi, 1, cols, dot(h_mid_t, err))
            total = total + dot(err, bi[high, :, cols], NT)
        dg[rows, :] = total.astype(bf16)
        return carry

    def sweep_back(i, carry):
        if perturbed:
            @pl.when(jnp.logical_and(i == 1, at.core == 1))
            def _():
                update()

        rows = block(i)
        h_low, d_mid = hg[rows, :], dg[rows, :]
        h_low_t, d_mid_t = h_low.T, d_mid.T

        def columns(cols):
            pre = us[rows, cols].astype(f32)
            half = cdf(pre)
            post = (pre * half).astype(bf16)
            err = (dot(d_mid, bo[low, cols, :], NT) * (half + slope_tail(pre))).astype(bf16)
            add(i, go, 0, cols, dot(d_mid_t, post))
            add(i, gi, 0, cols, dot(h_low_t, err))

        if perturbed:
            def part(p):
                for j in range(0, F // 2, KB_FT):
                    columns(pl.ds(pl.multiple_of(p * (F // 2) + j, KB_FT), KB_FT))

            each(0, 2, part)
        else:
            for j in range(0, F, KB_FT):
                columns(pl.ds(j, KB_FT))
        return carry

    def swap(which):
        return [remote(gi.at[which], ri, xsend.at[0], xrecv.at[0], at.partner()),
                remote(go.at[which], ro, xsend.at[1], xrecv.at[1], at.partner())]

    def squares(value, total):
        sq = value * value
        for r in range(0, sq.shape[0], 8):
            for q in range(0, sq.shape[1], 128):
                total = total + sq[r:r + 8, q:q + 128]
        return total

    R, C = 16, 128

    def sum_in(i, total):
        rows = pl.ds(pl.multiple_of(i * R, R), R)
        g = gi[at.core, rows, :] + ri[rows, :]
        if perturbed:
            wi[rows, :] = wi[rows, :] - LEARN_RATE * g
            return total
        ri[rows, :] = g
        return squares(g, total)

    def sum_out(i, total):
        cols = pl.ds(pl.multiple_of(i * C, C), C)
        g = go[at.core, :, cols] + ro[:, cols]
        if perturbed:
            wo[cols, :] = wo[cols, :] - LEARN_RATE * g.T
            return total
        ro[:, cols] = g
        return squares(g, total)

    def sum_layer():
        got = swap(0)
        got[0].wait_recv()
        total = lax.fori_loop(0, D // R, sum_in, jnp.zeros((8, 128), f32))
        got[1].wait_recv()
        return lax.fori_loop(0, F // C, sum_out, total)

    if perturbed:
        gather = Gather(at, [(wi, wi_out), (wo, wo_out)], gs, gr, gps, gpr)
        keep_new = [pltpu.make_async_copy(wi, wi_out.at[mine], wsem.at[0]), pltpu.make_async_copy(wo, wo_out.at[mine], wsem.at[1])]

    def update():
        wait(own_w)
        sum_layer()
        gather.start()
        start(keep_new)

    blocks = ROWS // KB_ROWS
    take(me * 2, low)
    lax.fori_loop(0, blocks, sweep_low, 0)
    take(me * 2 + 1, high)
    if not perturbed:
        start(own_w)
    lax.fori_loop(0, blocks, sweep_high, 0)

    @pl.when(at.core == 0)
    def _():
        start(swap(1))

    lax.fori_loop(0, blocks, sweep_back, 0)

    @pl.when(at.core == 1)
    def _():
        start(swap(0))

    def sent(t):
        moved(t, hs, hg, hsend, hrecv).wait_send()
        moved(t, ds, dg, dsend, drecv).wait_send()

    each(1, CHIPS, sent)
    if perturbed:
        @pl.when(at.core == 0)
        def _():
            update()

        gather.run()
        loss_out[...] = share_finish() * inv_count
        spread.finish()
        gather.finish()
        wait(keep_new)
    else:
        wait(own_w)
        sbuf[mine] = sum_layer()
        share_start()
        scale = radius / jnp.sqrt(jnp.sum(share_finish(), axis=(0, 1), keepdims=True))

        def perturb_in(i, carry):
            rows = pl.ds(pl.multiple_of(i * R, R), R)
            bi[0, rows, :] = (si[0, rows, :] + scale * ri[rows, :]).astype(bf16)
            return carry

        def perturb_out(i, carry):
            cols = pl.ds(pl.multiple_of(i * C, C), C)
            bo[0, cols, :] = (so[0, cols, :] + scale * ro[:, cols].T).astype(bf16)
            return carry

        lax.fori_loop(0, D // R, perturb_in, 0)
        lax.fori_loop(0, F // C, perturb_out, 0)
        done = [pltpu.make_async_copy(bi.at[0], wi_out, wsem.at[2]), pltpu.make_async_copy(bo.at[0], wo_out, wsem.at[3])]
        start(done)
        wait(done)
    for c in swap(0):
        c.wait_send()


def one_pass(perturbed, inv_count, radius, x, y, w_in, w_out, pert=()):
    acts = ((LAYERS, T, F), bf16)
    scratch = [
        pltpu.VMEM((2, D, F), bf16), pltpu.VMEM((2, F, D), bf16),
        pltpu.VMEM((ROWS + T, D), bf16), pltpu.VMEM((ROWS, D), bf16), pltpu.VMEM((ROWS, D), bf16), pltpu.VMEM((ROWS, F), bf16),
        pltpu.VMEM((ROWS, D), bf16), pltpu.VMEM((ROWS, D), bf16),
        pltpu.VMEM((2, D, F), f32), pltpu.VMEM((2, D, F), f32), pltpu.VMEM((D, F), f32), pltpu.VMEM((D, F), f32),
        DMA((CHIPS,)), DMA((CHIPS,)), DMA((CHIPS,)), DMA((CHIPS,)), DMA((KEPT,)), DMA((2, 2)), DMA((4,)), DMA((2,)), DMA((2,)),
        pltpu.VMEM((LAYERS, 8, 128), f32), DMA((LAYERS,)), DMA((LAYERS,)),
    ]
    if perturbed:
        shapes = [((LAYERS, D, F), f32), ((LAYERS, F, D), f32), ((LAYERS, D, F), bf16), ((LAYERS, F, D), bf16), acts, ((8, 128), f32)]
        out_specs = [ANY] * 5 + [V]
        scratch += [pltpu.VMEM((D, F), f32), pltpu.VMEM((F, D), f32), *GATHER_SEMS, *GATHER_SEMS]
    else:
        shapes = [((D, F), bf16), ((F, D), bf16), acts]
        out_specs = [ANY] * 3
        scratch += [pltpu.VMEM((2, D, F), f32), pltpu.VMEM((2, F, D), f32), DMA((2, 2))]
    options = dict(
        out_shape=[jax.ShapeDtypeStruct(*s) for s in shapes],
        in_specs=[V, V, ANY, ANY] + [V] * len(pert),
        out_specs=out_specs,
        scratch_shapes=scratch,
        compiler_params=pltpu.CompilerParams(
            collective_id=1 if perturbed else 0, has_side_effects=True, vmem_limit_bytes=VMEM_LIMIT),
        name="second_pass" if perturbed else "first_pass",
    )
    kernel = functools.partial(pass_kernel, perturbed, inv_count, radius)
    if perturbed:
        return pl.pallas_call(kernel, **options)(x, y, w_in, w_out, *pert)
    return pl.pallas_call(kernel, **options)(x, y, w_in, w_out)


def solution(mesh):
    mesh_axes = tuple(mesh.axis_names)
    dev_count = math.prod([mesh.shape[axis_name] for axis_name in mesh_axes])
    batch_spec = P(mesh_axes, None, None)

    def local_step(images, targets, w_in, w_out):
        layers, model_dim, hidden_dim = w_in.shape
        inv_count = 1.0 / (images.shape[0] * images.shape[1] * dev_count * model_dim)
        radius = RHO_REL * math.sqrt(layers * hidden_dim + model_dim)
        x, y = images.reshape(T, D), targets.reshape(T, D)
        pert = one_pass(False, inv_count, radius, x, y, w_in, w_out)[:2]
        new_in, new_out, _, _, _, loss = one_pass(True, inv_count, radius, x, y, w_in, w_out, pert)
        return new_in, new_out, loss[0, 0]

    return jax.shard_map(local_step, mesh=mesh, in_specs=(batch_spec, batch_spec, P(), P()), out_specs=(P(), P(), P()), check_vma=False)
```

```python
import functools
import math

import jax
import jax.numpy as jnp
from jax import lax
from jax.experimental import pallas as pl
from jax.experimental.pallas import tpu as pltpu
from jax.sharding import PartitionSpec as P

MESH = pl.DeviceIdType.MESH
RHO_REL = 0.1
LEARN_RATE = 8.0
SQRT_HALF = 0.7071067811865476
INV_SQRT_2PI = 0.3989422804014327
HALF_LOG2E = -0.7213475204444817

CHIPS = 8
LAYERS = 16
D = 384
F = 1536
T = 576
ROWS = CHIPS * T
FT = 768
KB_ROWS = 768
KB_FT = 256
KEPT = 8
PIECE = 144
VMEM_LIMIT = 67043328

f32, bf16 = jnp.float32, jnp.bfloat16
NN = (((1,), (0,)), ((), ()))
NT = (((1,), (1,)), ((), ()))
V = pl.BlockSpec(memory_space=pltpu.VMEM)
ANY = pl.BlockSpec(memory_space=pl.ANY)
DMA = pltpu.SemaphoreType.DMA


def dot(a, b, dims=NN):
    return lax.dot_general(a, b, dims, preferred_element_type=f32)


def cdf(x):
    return 0.5 * (1.0 + lax.erf(x * SQRT_HALF))


def slope_tail(x):
    return x * INV_SQRT_2PI * jnp.exp2((x * x) * HALF_LOG2E)


def div(a, b):
    return lax.div(jnp.int32(a), jnp.int32(b))


def rem(a, b):
    return lax.rem(jnp.int32(a), jnp.int32(b))


def some(k):
    return div(k * k + 35, 36)


def bit(dim):
    return 1 + dim + div(dim * (dim - 1), 2)


class Place:
    def __init__(self):
        self.z, self.y, data = lax.axis_index("model"), lax.axis_index("sub"), lax.axis_index("data")
        self.x, self.core = div(data, 2), rem(data, 2)
        self.chip = self.z * 4 + self.y * 2 + self.x
        self.mine = self.chip * 2 + self.core

    def across(self, t):
        x, y, z = rem(self.x + t, 2), rem(self.y + div(t, 2), 2), rem(self.z + div(t, 4), 2)
        return z * 4 + y * 2 + x

    def device(self, chip, core):
        return (div(chip, 4), rem(div(chip, 2), 2), rem(chip, 2) * 2 + core)

    def partner(self):
        return self.device(self.chip, 1 - self.core)

    def peer(self, i):
        return self.device(self.across(div(i, 2)), rem(self.core + i, 2))


def each(first, last, body):
    def step(i, carry):
        body(i)
        return carry

    lax.fori_loop(first, last, step, 0)


def greet(at):
    barrier = pltpu.get_barrier_semaphore()
    each(1, 16, lambda i: pl.semaphore_signal(barrier, inc=1, device_id=at.peer(i), device_id_type=MESH))


def met():
    pl.semaphore_wait(pltpu.get_barrier_semaphore(), 15)


def remote(src, dst, send_sem, recv_sem, device):
    return pltpu.make_async_remote_copy(
        src_ref=src, dst_ref=dst, send_sem=send_sem, recv_sem=recv_sem, device_id=device, device_id_type=MESH
    )


class Gather:
    def __init__(self, at, tensors, send, recv, pair_send, pair_recv):
        self.at, self.tensors = at, tensors
        self.sems = (send, recv, pair_send, pair_recv)

    def make(self, i, part, own, chip, send, recv, device):
        ref, slots = self.tensors[i]
        n = slots.shape[1] // 3
        rows = pl.ds(pl.multiple_of(part * n, n), n)
        dst = slots.at[chip * 2 + self.at.core, rows, :]
        return remote(ref.at[rows, :] if own else dst, dst, send, recv, device)

    def parts(self, dim, slot):
        later = some(slot) * some(slot - 1) * some(slot - 2)
        back = some(slot) + some(slot) * some(slot - 1) - 1 + some(slot - 3)
        one, two = later * some(slot - 4), later * (1 - rem(slot, 2))
        return rem(dim + 3 - back, 3), one * bit(rem(dim + 2, 3)) + two * bit(rem(dim + 1, 3))

    def link(self, i, dim, slot, own=False):
        part, t = (rem(dim + 3 - slot, 3), 0) if own else self.parts(dim, slot)
        send, recv, _, _ = self.sems
        index = slot * 3 + dim
        return self.make(i, part, own, self.at.chip if own else self.at.across(t), send.at[index, i], recv.at[index, i],
                         self.at.device(self.at.across(bit(dim)), self.at.core))

    def pair(self, i, part, own, chip, index):
        _, _, send, recv = self.sems
        return self.make(i, part, own, chip, send.at[index, i], recv.at[index, i], self.at.partner())

    def passing(self, i, index, which):
        return self.make(i, 0, False, self.at.chip, self.sems[which].at[index, i], self.sems[which + 1].at[index, i], self.at.partner())

    def start(self):
        def own(slot):
            for i in range(2):
                each(0, 3, lambda dim: self.link(i, dim, slot, own=True).start())

        each(0, 3, own)
        for i in range(2):
            each(0, 3, lambda part: self.pair(i, part, True, self.at.chip, part).start())

    def run(self):
        def step(slot):
            for i in range(2):
                def got(dim):
                    self.passing(i, slot * 3 + dim, 0).wait_recv()

                    @pl.when(jnp.logical_or(slot <= 1, slot == 3))
                    def _():
                        self.link(i, rem(dim + 1, 3), 3 + 2 * some(slot) + div(slot, 3)).start()

                    part, t = self.parts(dim, slot)
                    self.pair(i, part, False, self.at.across(t + bit(dim)), 3 + slot * 3 + dim).start()

                each(0, 3, got)

            @pl.when(slot == 0)
            def _():
                for i in range(2):
                    each(0, 3, lambda dim: self.link(i, dim, 4).start())

        each(0, 7, step)
        for i in range(2):
            each(0, 24, lambda index: self.passing(i, index, 2).wait_recv())

    def finish(self):
        for i in range(2):
            each(0, 24, lambda index: self.passing(i, index, 2).wait_send())
            each(0, 21, lambda index: self.passing(i, index, 0).wait_send())


GATHER_SEMS = [DMA((21, 2)), DMA((21, 2)), DMA((24, 2)), DMA((24, 2))]


def pass_kernel(perturbed, inv_count, radius, *refs):
    if perturbed:
        (x_ref, y_ref, wi_hbm, wo_hbm, wbi, wbo, wi_out, wo_out, u_hbm, loss_out,
         bi, bo, hs, ds, hm, us, hg, dg, gi, go, ri, ro,
         hsend, hrecv, dsend, drecv, usem, bsem, wsem, xsend, xrecv, sbuf, ssend, srecv,
         gs, gr, gps, gpr, wi, wo) = refs
    else:
        (x_ref, y_ref, wi_hbm, wo_hbm, wbi, wbo, u_hbm,
         bi, bo, hs, ds, hm, us, hg, dg, gi, go, ri, ro,
         hsend, hrecv, dsend, drecv, usem, bsem, wsem, xsend, xrecv, sbuf, ssend, srecv,
         gs, gr, gps, gpr, si, so, fsem) = refs
    at = Place()
    me = at.chip
    mine = at.mine

    def fetch32(layer, slot):
        return (pltpu.make_async_copy(wi_hbm.at[layer], si.at[slot], fsem.at[slot, 0]),
                pltpu.make_async_copy(wo_hbm.at[layer], so.at[slot], fsem.at[slot, 1]))

    def fetch16(layer, slot):
        return (pltpu.make_async_copy(wbi.at[layer], bi.at[slot], bsem.at[slot, 0]),
                pltpu.make_async_copy(wbo.at[layer], bo.at[slot], bsem.at[slot, 1]))

    fetch = fetch16 if perturbed else fetch32

    def start(copies):
        for c in copies:
            c.start()

    def wait(copies):
        for c in copies:
            c.wait()

    own_w = [pltpu.make_async_copy(wi_hbm.at[mine], wi if perturbed else si.at[0], wsem.at[0]),
             pltpu.make_async_copy(wo_hbm.at[mine], wo if perturbed else so.at[0], wsem.at[1])]
    for layer in range(2):
        start(fetch(layer, layer))
    if perturbed:
        start(own_w)
    greet(at)

    def span(k):
        return pl.ds(pl.multiple_of(k * T, T), T)

    def moved(t, src, dst, send_sem, recv_sem):
        chip = at.across(t)
        return remote(src.at[span(chip), :], dst.at[span(t), :], send_sem.at[t], recv_sem.at[t], at.device(chip, at.core))

    def exchange(src, dst, send_sem, recv_sem):
        for group in ((1, 2, 4), (3, 5, 6), (7,)):
            def step(q):
                for t in group:
                    chip = at.across(t)
                    remote(src.at[pl.ds(pl.multiple_of(chip * T + q * PIECE, 16), PIECE), :],
                           dst.at[pl.ds(pl.multiple_of(t * T + q * PIECE, 16), PIECE), :],
                           send_sem.at[t], recv_sem.at[t], at.device(chip, at.core)).start()

            each(0, T // PIECE, step)
        dst[pl.ds(0, T), :] = src[span(me), :]

    def weights(slot, cols):
        if perturbed:
            return bi[slot, :, cols], bo[slot, cols, :]
        return si[slot, :, cols].astype(bf16), so[slot, cols, :].astype(bf16)

    def kept(layer):
        return us.at[span(layer % KEPT), :]

    def put(layer):
        return pltpu.make_async_copy(kept(layer), u_hbm.at[layer], usem.at[layer % KEPT])

    def get(layer):
        return pltpu.make_async_copy(u_hbm.at[layer], kept(layer), usem.at[layer % KEPT])

    def layer_forward(layer, carry):
        slot = layer % 2
        hidden = hs[span((layer + 1) // 2), :]
        pre_out = kept(layer)

        @pl.when(layer >= KEPT + 2)
        def _():
            put(layer - KEPT).wait()

        wait(fetch(layer, slot))
        total = hidden.astype(f32)
        for j in range(0, F, FT):
            cols = pl.ds(j, FT)
            a_w, b_w = weights(slot, cols)
            pre = dot(hidden, a_w).astype(bf16)
            pre_out[:, cols] = pre
            pre = pre.astype(f32)
            total = total + dot((pre * cdf(pre)).astype(bf16), b_w)

        @pl.when(jnp.logical_and(layer >= 2, layer < KEPT))
        def _():
            put(layer).start()

        @pl.when(layer < LAYERS - 2)
        def _():
            start(fetch(layer + 2, slot))

        hs[span((layer + 2) // 2), :] = total.astype(bf16)
        return carry

    hs[pl.ds(0, T), :] = x_ref[...]
    lax.fori_loop(0, LAYERS, layer_forward, 0)
    met()
    exchange(hs, hg, hsend, hrecv)

    def share(value):
        sbuf[mine] = jnp.broadcast_to(value, (8, 128))

    def shared(i):
        return remote(sbuf.at[mine], sbuf.at[mine], ssend.at[i], srecv.at[mine], at.peer(i))

    def share_start():
        each(1, LAYERS, lambda i: shared(i).start())

    def share_finish():
        each(1, LAYERS, lambda i: shared(i).wait_send())

        def gathered(i):
            @pl.when(i != mine)
            def _():
                remote(sbuf.at[i], sbuf.at[i], ssend.at[0], srecv.at[i], at.partner()).wait_recv()

        each(0, LAYERS, gathered)
        total = sbuf[0]
        for i in range(1, LAYERS):
            total = total + sbuf[i]
        return total

    resid = hs[pl.ds(CHIPS * T, T), :].astype(f32) - y_ref[...].astype(f32)
    ds[pl.ds((CHIPS - 1) * T, T), :] = (resid * inv_count).astype(bf16)
    if perturbed:
        share(0.5 * jnp.sum(resid * resid, axis=(0, 1), keepdims=True))

    def layer_backward(i, carry):
        layer = LAYERS - 1 - i
        slot = layer % 2
        cot = ds[span((layer - 1) // 2), :]
        pre_in = kept(layer)

        @pl.when(layer < KEPT)
        def _():
            get(layer).wait()

        @pl.when(layer < LAYERS - 2)
        def _():
            wait(fetch(layer, slot))

        total = cot.astype(f32)
        for j in range(0, F, FT):
            cols = pl.ds(j, FT)
            a_w, b_w = weights(slot, cols)
            pre = pre_in[:, cols].astype(f32)
            err = (dot(cot, b_w, NT) * (cdf(pre) + slope_tail(pre))).astype(bf16)
            total = total + dot(err, a_w, NT)

        @pl.when(layer >= KEPT + 2)
        def _():
            get(layer - KEPT).start()

        @pl.when(layer >= 4)
        def _():
            start(fetch(layer - 2, slot))

        @pl.when(layer < 4)
        def _():
            start(fetch(me * 2 + 3 - layer, slot))

        ds[span((layer - 2) // 2), :] = total.astype(bf16)
        return carry

    lax.fori_loop(0, LAYERS - 2, layer_backward, 0)
    exchange(ds, dg, dsend, drecv)
    if perturbed:
        share_start()
    low, high = 1, 0

    def take(layer, slot):
        wait(fetch(layer, slot))
        if not perturbed:
            for j in range(0, F, FT):
                cols = pl.ds(j, FT)
                bi[slot, :, cols], bo[slot, cols, :] = weights(slot, cols)

    def block(i):
        return pl.ds(pl.multiple_of(i * KB_ROWS, KB_ROWS), KB_ROWS)

    def arrive(i, src, dst, send_sem, recv_sem):
        def step(t):
            @pl.when(t * T // KB_ROWS == i)
            def _():
                moved(t, src, dst, send_sem, recv_sem).wait_recv()

        each(1, CHIPS, step)

    def add(i, ref, which, cols, value):
        ref[which, :, cols] = jnp.where(i == 0, 0.0, ref[which, :, cols]) + value

    def sweep_low(i, carry):
        arrive(i, hs, hg, hsend, hrecv)
        rows = block(i)
        h_low = hg[rows, :]
        total = h_low.astype(f32)
        for j in range(0, F, FT):
            cols = pl.ds(j, FT)
            pre = dot(h_low, bi[low, :, cols]).astype(bf16)
            us[rows, cols] = pre
            pre = pre.astype(f32)
            total = total + dot((pre * cdf(pre)).astype(bf16), bo[low, cols, :])
        hm[rows, :] = total.astype(bf16)
        return carry

    def sweep_high(i, carry):
        arrive(i, ds, dg, dsend, drecv)
        rows = block(i)
        h_mid, d_top = hm[rows, :], dg[rows, :]
        h_mid_t, d_top_t = h_mid.T, d_top.T
        total = d_top.astype(f32)
        for j in range(0, F, KB_FT):
            cols = pl.ds(j, KB_FT)
            pre = dot(h_mid, bi[high, :, cols]).astype(bf16).astype(f32)
            half = cdf(pre)
            post = (pre * half).astype(bf16)
            err = (dot(d_top, bo[high, cols, :], NT) * (half + slope_tail(pre))).astype(bf16)
            add(i, go, 1, cols, dot(d_top_t, post))
            add(i, gi, 1, cols, dot(h_mid_t, err))
            total = total + dot(err, bi[high, :, cols], NT)
        dg[rows, :] = total.astype(bf16)
        return carry

    def sweep_back(i, carry):
        if perturbed:
            @pl.when(jnp.logical_and(i == 1, at.core == 1))
            def _():
                update()

        rows = block(i)
        h_low, d_mid = hg[rows, :], dg[rows, :]
        h_low_t, d_mid_t = h_low.T, d_mid.T

        def columns(cols):
            pre = us[rows, cols].astype(f32)
            half = cdf(pre)
            post = (pre * half).astype(bf16)
            err = (dot(d_mid, bo[low, cols, :], NT) * (half + slope_tail(pre))).astype(bf16)
            add(i, go, 0, cols, dot(d_mid_t, post))
            add(i, gi, 0, cols, dot(h_low_t, err))

        if perturbed:
            def part(p):
                for j in range(0, F // 2, KB_FT):
                    columns(pl.ds(pl.multiple_of(p * (F // 2) + j, KB_FT), KB_FT))

            each(0, 2, part)
        else:
            for j in range(0, F, KB_FT):
                columns(pl.ds(j, KB_FT))
        return carry

    def swap(which):
        return [remote(gi.at[which], ri, xsend.at[0], xrecv.at[0], at.partner()),
                remote(go.at[which], ro, xsend.at[1], xrecv.at[1], at.partner())]

    def squares(value, total):
        sq = value * value
        for r in range(0, sq.shape[0], 8):
            for q in range(0, sq.shape[1], 128):
                total = total + sq[r:r + 8, q:q + 128]
        return total

    R, C = 16, 128

    def sum_in(i, total):
        rows = pl.ds(pl.multiple_of(i * R, R), R)
        g = gi[at.core, rows, :] + ri[rows, :]
        if perturbed:
            wi[rows, :] = wi[rows, :] - LEARN_RATE * g
            return total
        ri[rows, :] = g
        return squares(g, total)

    def sum_out(i, total):
        cols = pl.ds(pl.multiple_of(i * C, C), C)
        g = go[at.core, :, cols] + ro[:, cols]
        if perturbed:
            wo[cols, :] = wo[cols, :] - LEARN_RATE * g.T
            return total
        ro[:, cols] = g
        return squares(g, total)

    def sum_layer():
        got = swap(0)
        got[0].wait_recv()
        total = lax.fori_loop(0, D // R, sum_in, jnp.zeros((8, 128), f32))
        got[1].wait_recv()
        return lax.fori_loop(0, F // C, sum_out, total)

    if perturbed:
        new = [(wi, wi_out), (wo, wo_out)]
    else:
        new = [(bi.at[0], wbi), (bo.at[0], wbo)]
    gather = Gather(at, new, gs, gr, gps, gpr)
    keep_new = [pltpu.make_async_copy(own, slots.at[mine], wsem.at[2 + i]) for i, (own, slots) in enumerate(new)]

    def update():
        wait(own_w)
        sum_layer()
        gather.start()
        start(keep_new)

    blocks = ROWS // KB_ROWS
    take(me * 2, low)
    lax.fori_loop(0, blocks, sweep_low, 0)
    take(me * 2 + 1, high)
    if not perturbed:
        start(own_w)
    lax.fori_loop(0, blocks, sweep_high, 0)

    @pl.when(at.core == 0)
    def _():
        start(swap(1))

    lax.fori_loop(0, blocks, sweep_back, 0)

    @pl.when(at.core == 1)
    def _():
        start(swap(0))

    def sent(t):
        moved(t, hs, hg, hsend, hrecv).wait_send()
        moved(t, ds, dg, dsend, drecv).wait_send()

    each(1, CHIPS, sent)
    if perturbed:
        @pl.when(at.core == 0)
        def _():
            update()

        loss_out[0] = jnp.max(share_finish() * inv_count)
    else:
        wait(own_w)
        sbuf[mine] = sum_layer()
        share_start()
        scale = radius / jnp.sqrt(jnp.sum(share_finish(), axis=(0, 1), keepdims=True))

        def perturb_in(i, carry):
            rows = pl.ds(pl.multiple_of(i * R, R), R)
            bi[0, rows, :] = (si[0, rows, :] + scale * ri[rows, :]).astype(bf16)
            return carry

        def perturb_out(i, carry):
            cols = pl.ds(pl.multiple_of(i * C, C), C)
            bo[0, cols, :] = (so[0, cols, :] + scale * ro[:, cols].T).astype(bf16)
            return carry

        lax.fori_loop(0, D // R, perturb_in, 0)
        lax.fori_loop(0, F // C, perturb_out, 0)
        gather.start()
        start(keep_new)

    gather.run()
    gather.finish()
    wait(keep_new)
    for c in swap(0):
        c.wait_send()


def one_pass(perturbed, inv_count, radius, x, y, w_in, w_out, pert=()):
    acts = ((LAYERS, T, F), bf16)
    scratch = [
        pltpu.VMEM((2, D, F), bf16), pltpu.VMEM((2, F, D), bf16),
        pltpu.VMEM((ROWS + T, D), bf16), pltpu.VMEM((ROWS, D), bf16), pltpu.VMEM((ROWS, D), bf16), pltpu.VMEM((ROWS, F), bf16),
        pltpu.VMEM((ROWS, D), bf16), pltpu.VMEM((ROWS, D), bf16),
        pltpu.VMEM((2, D, F), f32), pltpu.VMEM((2, D, F), f32), pltpu.VMEM((D, F), f32), pltpu.VMEM((D, F), f32),
        DMA((CHIPS,)), DMA((CHIPS,)), DMA((CHIPS,)), DMA((CHIPS,)), DMA((KEPT,)), DMA((2, 2)), DMA((4,)), DMA((2,)), DMA((2,)),
        pltpu.VMEM((LAYERS, 8, 128), f32), DMA((LAYERS,)), DMA((LAYERS,)),
    ]
    if perturbed:
        shapes = [((LAYERS, D, F), f32), ((LAYERS, F, D), f32), acts, ((1,), f32)]
        out_specs = [ANY] * 3 + [pl.BlockSpec(memory_space=pltpu.SMEM)]
        scratch += [*GATHER_SEMS, pltpu.VMEM((D, F), f32), pltpu.VMEM((F, D), f32)]
    else:
        shapes = [((LAYERS, D, F), bf16), ((LAYERS, F, D), bf16), acts]
        out_specs = [ANY] * 3
        scratch += [*GATHER_SEMS, pltpu.VMEM((2, D, F), f32), pltpu.VMEM((2, F, D), f32), DMA((2, 2))]
    options = dict(
        out_shape=[jax.ShapeDtypeStruct(*s) for s in shapes],
        in_specs=[V, V, ANY, ANY] + [ANY] * len(pert),
        out_specs=out_specs,
        scratch_shapes=scratch,
        compiler_params=pltpu.CompilerParams(
            collective_id=1 if perturbed else 0, has_side_effects=True, vmem_limit_bytes=VMEM_LIMIT),
        name="second_pass" if perturbed else "first_pass",
    )
    kernel = functools.partial(pass_kernel, perturbed, inv_count, radius)
    if perturbed:
        return pl.pallas_call(kernel, **options)(x, y, w_in, w_out, *pert)
    return pl.pallas_call(kernel, **options)(x, y, w_in, w_out)


def solution(mesh):
    mesh_axes = tuple(mesh.axis_names)
    dev_count = math.prod([mesh.shape[axis_name] for axis_name in mesh_axes])
    batch_spec = P(mesh_axes, None, None)

    def local_step(images, targets, w_in, w_out):
        layers, model_dim, hidden_dim = w_in.shape
        inv_count = 1.0 / (images.shape[0] * images.shape[1] * dev_count * model_dim)
        radius = RHO_REL * math.sqrt(layers * hidden_dim + model_dim)
        x, y = images.reshape(T, D), targets.reshape(T, D)
        pert = one_pass(False, inv_count, radius, x, y, w_in, w_out)[:2]
        new_in, new_out, _, loss = one_pass(True, inv_count, radius, x, y, w_in, w_out, pert)
        return new_in, new_out, loss.reshape(())

    return jax.shard_map(local_step, mesh=mesh, in_specs=(batch_spec, batch_spec, P(), P()), out_specs=(P(), P(), P()), check_vma=False)
```

```python
import functools
import math

import jax
import jax.numpy as jnp
from jax import lax
from jax.experimental import pallas as pl
from jax.experimental.pallas import tpu as pltpu
from jax.sharding import PartitionSpec as P

MESH = pl.DeviceIdType.MESH
RHO_REL = 0.1
LEARN_RATE = 8.0
SQRT_HALF = 0.7071067811865476
INV_SQRT_2PI = 0.3989422804014327
HALF_LOG2E = -0.7213475204444817

CHIPS = 8
LAYERS = 16
D = 384
F = 1536
T = 576
ROWS = CHIPS * T
FT = 768
KB_ROWS = 768
KB_FT = 256
KEPT = 8
PIECE = 144
VMEM_LIMIT = 67043328

f32, bf16 = jnp.float32, jnp.bfloat16
NN = (((1,), (0,)), ((), ()))
NT = (((1,), (1,)), ((), ()))
V = pl.BlockSpec(memory_space=pltpu.VMEM)
ANY = pl.BlockSpec(memory_space=pl.ANY)
DMA = pltpu.SemaphoreType.DMA


def dot(a, b, dims=NN):
    return lax.dot_general(a, b, dims, preferred_element_type=f32)


def cdf(x):
    return 0.5 * (1.0 + lax.erf(x * SQRT_HALF))


def slope_tail(x):
    return x * INV_SQRT_2PI * jnp.exp2((x * x) * HALF_LOG2E)


def div(a, b):
    return lax.div(jnp.int32(a), jnp.int32(b))


def rem(a, b):
    return lax.rem(jnp.int32(a), jnp.int32(b))


def some(k):
    return div(k * k + 35, 36)


def bit(dim):
    return 1 + dim + div(dim * (dim - 1), 2)


class Place:
    def __init__(self):
        self.z, self.y, data = lax.axis_index("model"), lax.axis_index("sub"), lax.axis_index("data")
        self.x, self.core = div(data, 2), rem(data, 2)
        self.chip = self.z * 4 + self.y * 2 + self.x
        self.mine = self.chip * 2 + self.core

    def across(self, t):
        x, y, z = rem(self.x + t, 2), rem(self.y + div(t, 2), 2), rem(self.z + div(t, 4), 2)
        return z * 4 + y * 2 + x

    def device(self, chip, core):
        return (div(chip, 4), rem(div(chip, 2), 2), rem(chip, 2) * 2 + core)

    def partner(self):
        return self.device(self.chip, 1 - self.core)

    def peer(self, i):
        return self.device(self.across(div(i, 2)), rem(self.core + i, 2))


def each(first, last, body):
    def step(i, carry):
        body(i)
        return carry

    lax.fori_loop(first, last, step, 0)


def greet(at):
    barrier = pltpu.get_barrier_semaphore()
    each(1, 16, lambda i: pl.semaphore_signal(barrier, inc=1, device_id=at.peer(i), device_id_type=MESH))


def met():
    pl.semaphore_wait(pltpu.get_barrier_semaphore(), 15)


def remote(src, dst, send_sem, recv_sem, device):
    return pltpu.make_async_remote_copy(
        src_ref=src, dst_ref=dst, send_sem=send_sem, recv_sem=recv_sem, device_id=device, device_id_type=MESH
    )


class Gather:
    def __init__(self, at, tensors, send, recv, pair_send, pair_recv):
        self.at, self.tensors = at, tensors
        self.sems = (send, recv, pair_send, pair_recv)

    def make(self, i, part, own, chip, send, recv, device):
        ref, slots = self.tensors[i]
        n = slots.shape[1] // 3
        rows = pl.ds(pl.multiple_of(part * n, n), n)
        dst = slots.at[chip * 2 + self.at.core, rows, :]
        return remote(ref.at[rows, :] if own else dst, dst, send, recv, device)

    def parts(self, dim, slot):
        later = some(slot) * some(slot - 1) * some(slot - 2)
        back = some(slot) + some(slot) * some(slot - 1) - 1 + some(slot - 3)
        one, two = later * some(slot - 4), later * (1 - rem(slot, 2))
        return rem(dim + 3 - back, 3), one * bit(rem(dim + 2, 3)) + two * bit(rem(dim + 1, 3))

    def link(self, i, dim, slot, own=False):
        part, t = (rem(dim + 3 - slot, 3), 0) if own else self.parts(dim, slot)
        send, recv, _, _ = self.sems
        index = slot * 3 + dim
        return self.make(i, part, own, self.at.chip if own else self.at.across(t), send.at[index, i], recv.at[index, i],
                         self.at.device(self.at.across(bit(dim)), self.at.core))

    def pair(self, i, part, own, chip, index):
        _, _, send, recv = self.sems
        return self.make(i, part, own, chip, send.at[index, i], recv.at[index, i], self.at.partner())

    def passing(self, i, index, which):
        return self.make(i, 0, False, self.at.chip, self.sems[which].at[index, i], self.sems[which + 1].at[index, i], self.at.partner())

    def start(self):
        def own(slot):
            for i in range(2):
                each(0, 3, lambda dim: self.link(i, dim, slot, own=True).start())

        each(0, 3, own)
        for i in range(2):
            each(0, 3, lambda part: self.pair(i, part, True, self.at.chip, part).start())

    def run(self):
        def step(slot):
            for i in range(2):
                def got(dim):
                    self.passing(i, slot * 3 + dim, 0).wait_recv()

                    @pl.when(jnp.logical_or(slot <= 1, slot == 3))
                    def _():
                        self.link(i, rem(dim + 1, 3), 3 + 2 * some(slot) + div(slot, 3)).start()

                    part, t = self.parts(dim, slot)
                    self.pair(i, part, False, self.at.across(t + bit(dim)), 3 + slot * 3 + dim).start()

                each(0, 3, got)

            @pl.when(slot == 0)
            def _():
                for i in range(2):
                    each(0, 3, lambda dim: self.link(i, dim, 4).start())

        each(0, 7, step)
        for i in range(2):
            each(0, 24, lambda index: self.passing(i, index, 2).wait_recv())

    def finish(self):
        for i in range(2):
            each(0, 24, lambda index: self.passing(i, index, 2).wait_send())
            each(0, 21, lambda index: self.passing(i, index, 0).wait_send())


GATHER_SEMS = [DMA((21, 2)), DMA((21, 2)), DMA((24, 2)), DMA((24, 2))]


def pass_kernel(perturbed, inv_count, radius, *refs):
    if perturbed:
        (x_ref, y_ref, wi_hbm, wo_hbm, wbi, wbo, wi_out, wo_out, u_hbm, loss_out,
         bi, bo, hs, ds, hm, us, hg, dg, gi, go, ri, ro,
         hsend, hrecv, dsend, drecv, usem, bsem, wsem, xsend, xrecv, sbuf, ssend, srecv,
         gs, gr, gps, gpr, wi, wo) = refs
    else:
        (x_ref, y_ref, wi_hbm, wo_hbm, wbi, wbo, u_hbm,
         bi, bo, hs, ds, hm, us, hg, dg, gi, go, ri, ro,
         hsend, hrecv, dsend, drecv, usem, bsem, wsem, xsend, xrecv, sbuf, ssend, srecv,
         gs, gr, gps, gpr, si, so, fsem) = refs
    at = Place()
    me = at.chip
    mine = at.mine

    def fetch32(layer, slot):
        return (pltpu.make_async_copy(wi_hbm.at[layer], si.at[slot], fsem.at[slot, 0]),
                pltpu.make_async_copy(wo_hbm.at[layer], so.at[slot], fsem.at[slot, 1]))

    def fetch16(layer, slot):
        return (pltpu.make_async_copy(wbi.at[layer], bi.at[slot], bsem.at[slot, 0]),
                pltpu.make_async_copy(wbo.at[layer], bo.at[slot], bsem.at[slot, 1]))

    fetch = fetch16 if perturbed else fetch32

    def start(copies):
        for c in copies:
            c.start()

    def wait(copies):
        for c in copies:
            c.wait()

    own_w = [pltpu.make_async_copy(wi_hbm.at[mine], wi if perturbed else si.at[0], wsem.at[0]),
             pltpu.make_async_copy(wo_hbm.at[mine], wo if perturbed else so.at[0], wsem.at[1])]
    for layer in range(2):
        start(fetch(layer, layer))
    if perturbed:
        start(own_w)
    greet(at)

    def span(k):
        return pl.ds(pl.multiple_of(k * T, T), T)

    def moved(t, src, dst, send_sem, recv_sem):
        chip = at.across(t)
        return remote(src.at[span(chip), :], dst.at[span(t), :], send_sem.at[t], recv_sem.at[t], at.device(chip, at.core))

    def exchange(src, dst, send_sem, recv_sem):
        for group in ((1, 2, 4), (3, 5, 6), (7,)):
            def step(q):
                for t in group:
                    chip = at.across(t)
                    remote(src.at[pl.ds(pl.multiple_of(chip * T + q * PIECE, 16), PIECE), :],
                           dst.at[pl.ds(pl.multiple_of(t * T + q * PIECE, 16), PIECE), :],
                           send_sem.at[t], recv_sem.at[t], at.device(chip, at.core)).start()

            each(0, T // PIECE, step)
        dst[pl.ds(0, T), :] = src[span(me), :]

    def weights(slot, cols):
        if perturbed:
            return bi[slot, :, cols], bo[slot, cols, :]
        return si[slot, :, cols].astype(bf16), so[slot, cols, :].astype(bf16)

    def kept(layer):
        return us.at[span(layer % KEPT), :]

    def put(layer):
        return pltpu.make_async_copy(kept(layer), u_hbm.at[layer], usem.at[layer % KEPT])

    def get(layer):
        return pltpu.make_async_copy(u_hbm.at[layer], kept(layer), usem.at[layer % KEPT])

    def layer_forward(layer, carry):
        slot = layer % 2
        hidden = hs[span((layer + 1) // 2), :]
        pre_out = kept(layer)

        @pl.when(layer >= KEPT + 2)
        def _():
            put(layer - KEPT).wait()

        wait(fetch(layer, slot))
        total = hidden.astype(f32)
        for j in range(0, F, FT):
            cols = pl.ds(j, FT)
            a_w, b_w = weights(slot, cols)
            pre = dot(hidden, a_w).astype(bf16)
            pre_out[:, cols] = pre
            pre = pre.astype(f32)
            total = total + dot((pre * cdf(pre)).astype(bf16), b_w)

        @pl.when(jnp.logical_and(layer >= 2, layer < KEPT))
        def _():
            put(layer).start()

        @pl.when(layer < LAYERS - 2)
        def _():
            start(fetch(layer + 2, slot))

        hs[span((layer + 2) // 2), :] = total.astype(bf16)
        return carry

    hs[pl.ds(0, T), :] = x_ref[...]
    lax.fori_loop(0, LAYERS, layer_forward, 0)
    met()
    exchange(hs, hg, hsend, hrecv)

    def share(value):
        sbuf[mine] = jnp.broadcast_to(value, (8, 128))

    def shared(i):
        return remote(sbuf.at[mine], sbuf.at[mine], ssend.at[i], srecv.at[mine], at.peer(i))

    def share_start():
        each(1, LAYERS, lambda i: shared(i).start())

    def share_finish():
        each(1, LAYERS, lambda i: shared(i).wait_send())

        def gathered(i):
            @pl.when(i != mine)
            def _():
                remote(sbuf.at[i], sbuf.at[i], ssend.at[0], srecv.at[i], at.partner()).wait_recv()

        each(0, LAYERS, gathered)
        total = sbuf[0]
        for i in range(1, LAYERS):
            total = total + sbuf[i]
        return total

    resid = hs[pl.ds(CHIPS * T, T), :].astype(f32) - y_ref[...].astype(f32)
    ds[pl.ds((CHIPS - 1) * T, T), :] = (resid * inv_count).astype(bf16)
    if perturbed:
        share(0.5 * jnp.sum(resid * resid, axis=(0, 1), keepdims=True))

    def layer_backward(i, carry):
        layer = LAYERS - 1 - i
        slot = layer % 2
        cot = ds[span((layer - 1) // 2), :]
        pre_in = kept(layer)

        @pl.when(layer < KEPT)
        def _():
            get(layer).wait()

        @pl.when(layer < LAYERS - 2)
        def _():
            wait(fetch(layer, slot))

        total = cot.astype(f32)
        for j in range(0, F, FT):
            cols = pl.ds(j, FT)
            a_w, b_w = weights(slot, cols)
            pre = pre_in[:, cols].astype(f32)
            err = (dot(cot, b_w, NT) * (cdf(pre) + slope_tail(pre))).astype(bf16)
            total = total + dot(err, a_w, NT)

        @pl.when(layer >= KEPT + 2)
        def _():
            get(layer - KEPT).start()

        @pl.when(layer >= 4)
        def _():
            start(fetch(layer - 2, slot))

        @pl.when(layer < 4)
        def _():
            start(fetch(me * 2 + 3 - layer, slot))

        ds[span((layer - 2) // 2), :] = total.astype(bf16)
        return carry

    lax.fori_loop(0, LAYERS - 2, layer_backward, 0)
    exchange(ds, dg, dsend, drecv)
    if perturbed:
        share_start()
    low, high = 1, 0

    def take(layer, slot):
        wait(fetch(layer, slot))
        if not perturbed:
            for j in range(0, F, FT):
                cols = pl.ds(j, FT)
                bi[slot, :, cols], bo[slot, cols, :] = weights(slot, cols)

    def block(i):
        return pl.ds(pl.multiple_of(i * KB_ROWS, KB_ROWS), KB_ROWS)

    def arrive(i, src, dst, send_sem, recv_sem):
        def step(t):
            @pl.when(t * T // KB_ROWS == i)
            def _():
                moved(t, src, dst, send_sem, recv_sem).wait_recv()

        each(1, CHIPS, step)

    def add(i, ref, which, cols, value):
        ref[which, :, cols] = jnp.where(i == 0, 0.0, ref[which, :, cols]) + value

    def sweep_low(i, carry):
        arrive(i, hs, hg, hsend, hrecv)
        rows = block(i)
        h_low = hg[rows, :]
        total = h_low.astype(f32)
        for j in range(0, F, FT):
            cols = pl.ds(j, FT)
            pre = dot(h_low, bi[low, :, cols]).astype(bf16)
            us[rows, cols] = pre
            pre = pre.astype(f32)
            total = total + dot((pre * cdf(pre)).astype(bf16), bo[low, cols, :])
        hm[rows, :] = total.astype(bf16)
        return carry

    def sweep_high(i, carry):
        arrive(i, ds, dg, dsend, drecv)
        rows = block(i)
        h_mid, d_top = hm[rows, :], dg[rows, :]
        h_mid_t, d_top_t = h_mid.T, d_top.T
        total = d_top.astype(f32)
        for j in range(0, F, KB_FT):
            cols = pl.ds(j, KB_FT)
            pre = dot(h_mid, bi[high, :, cols]).astype(bf16).astype(f32)
            half = cdf(pre)
            post = (pre * half).astype(bf16)
            err = (dot(d_top, bo[high, cols, :], NT) * (half + slope_tail(pre))).astype(bf16)
            add(i, go, 1, cols, dot(d_top_t, post))
            add(i, gi, 1, cols, dot(h_mid_t, err))
            total = total + dot(err, bi[high, :, cols], NT)
        dg[rows, :] = total.astype(bf16)
        return carry

    def sweep_back(i, carry):
        if perturbed:
            @pl.when(jnp.logical_and(i == 1, at.core == 1))
            def _():
                update()

        rows = block(i)
        h_low, d_mid = hg[rows, :], dg[rows, :]
        h_low_t, d_mid_t = h_low.T, d_mid.T

        def columns(cols):
            pre = us[rows, cols].astype(f32)
            half = cdf(pre)
            post = (pre * half).astype(bf16)
            err = (dot(d_mid, bo[low, cols, :], NT) * (half + slope_tail(pre))).astype(bf16)
            add(i, go, 0, cols, dot(d_mid_t, post))
            add(i, gi, 0, cols, dot(h_low_t, err))

        if perturbed:
            def part(p):
                for j in range(0, F // 2, KB_FT):
                    columns(pl.ds(pl.multiple_of(p * (F // 2) + j, KB_FT), KB_FT))

            each(0, 2, part)
        else:
            for j in range(0, F, KB_FT):
                columns(pl.ds(j, KB_FT))
        return carry

    def swap(which):
        return [remote(gi.at[which], ri, xsend.at[0], xrecv.at[0], at.partner()),
                remote(go.at[which], ro, xsend.at[1], xrecv.at[1], at.partner())]

    def squares(value, total):
        sq = value * value
        for r in range(0, sq.shape[0], 8):
            for q in range(0, sq.shape[1], 128):
                total = total + sq[r:r + 8, q:q + 128]
        return total

    R, C = 16, 128

    def sum_in(i, total):
        rows = pl.ds(pl.multiple_of(i * R, R), R)
        g = gi[at.core, rows, :] + ri[rows, :]
        if perturbed:
            wi[rows, :] = wi[rows, :] - LEARN_RATE * g
            return total
        ri[rows, :] = g
        return squares(g, total)

    def sum_out(i, total):
        cols = pl.ds(pl.multiple_of(i * C, C), C)
        g = go[at.core, :, cols] + ro[:, cols]
        if perturbed:
            wo[cols, :] = wo[cols, :] - LEARN_RATE * g.T
            return total
        ro[:, cols] = g
        return squares(g, total)

    def sum_layer():
        got = swap(0)
        got[0].wait_recv()
        total = lax.fori_loop(0, D // R, sum_in, jnp.zeros((8, 128), f32))
        got[1].wait_recv()
        return lax.fori_loop(0, F // C, sum_out, total)

    if perturbed:
        new = [(wi, wi_out), (wo, wo_out)]
    else:
        new = [(bi.at[0], wbi), (bo.at[0], wbo)]
    gather = Gather(at, new, gs, gr, gps, gpr)
    keep_new = [pltpu.make_async_copy(own, slots.at[mine], wsem.at[2 + i]) for i, (own, slots) in enumerate(new)]

    def update():
        wait(own_w)
        sum_layer()
        gather.start()
        start(keep_new)

    blocks = ROWS // KB_ROWS
    take(me * 2, low)
    lax.fori_loop(0, blocks, sweep_low, 0)
    take(me * 2 + 1, high)
    if not perturbed:
        start(own_w)
    lax.fori_loop(0, blocks, sweep_high, 0)

    @pl.when(at.core == 0)
    def _():
        start(swap(1))

    lax.fori_loop(0, blocks, sweep_back, 0)

    @pl.when(at.core == 1)
    def _():
        start(swap(0))

    def sent(t):
        moved(t, hs, hg, hsend, hrecv).wait_send()
        moved(t, ds, dg, dsend, drecv).wait_send()

    each(1, CHIPS, sent)
    if perturbed:
        @pl.when(at.core == 0)
        def _():
            update()

        loss_out[0] = jnp.max(share_finish() * inv_count)
    else:
        wait(own_w)
        sbuf[mine] = sum_layer()
        share_start()

        def turn(i, carry):
            cols = pl.ds(pl.multiple_of(i * C, C), C)
            so[1, cols, :] = ro[:, cols].T
            return carry

        lax.fori_loop(0, F // C, turn, 0)
        scale = radius / jnp.sqrt(jnp.sum(share_finish(), axis=(0, 1), keepdims=True))

        def perturb_in(i, carry):
            rows = pl.ds(pl.multiple_of(i * R, R), R)
            bi[0, rows, :] = (si[0, rows, :] + scale * ri[rows, :]).astype(bf16)
            return carry

        def perturb_out(i, carry):
            cols = pl.ds(pl.multiple_of(i * C, C), C)
            bo[0, cols, :] = (so[0, cols, :] + scale * so[1, cols, :]).astype(bf16)
            return carry

        lax.fori_loop(0, D // R, perturb_in, 0)
        lax.fori_loop(0, F // C, perturb_out, 0)
        gather.start()
        start(keep_new)

    gather.run()
    gather.finish()
    wait(keep_new)
    for c in swap(0):
        c.wait_send()


def one_pass(perturbed, inv_count, radius, x, y, w_in, w_out, pert=()):
    acts = ((LAYERS, T, F), bf16)
    scratch = [
        pltpu.VMEM((2, D, F), bf16), pltpu.VMEM((2, F, D), bf16),
        pltpu.VMEM((ROWS + T, D), bf16), pltpu.VMEM((ROWS, D), bf16), pltpu.VMEM((ROWS, D), bf16), pltpu.VMEM((ROWS, F), bf16),
        pltpu.VMEM((ROWS, D), bf16), pltpu.VMEM((ROWS, D), bf16),
        pltpu.VMEM((2, D, F), f32), pltpu.VMEM((2, D, F), f32), pltpu.VMEM((D, F), f32), pltpu.VMEM((D, F), f32),
        DMA((CHIPS,)), DMA((CHIPS,)), DMA((CHIPS,)), DMA((CHIPS,)), DMA((KEPT,)), DMA((2, 2)), DMA((4,)), DMA((2,)), DMA((2,)),
        pltpu.VMEM((LAYERS, 8, 128), f32), DMA((LAYERS,)), DMA((LAYERS,)),
    ]
    if perturbed:
        shapes = [((LAYERS, D, F), f32), ((LAYERS, F, D), f32), acts, ((1,), f32)]
        out_specs = [ANY] * 3 + [pl.BlockSpec(memory_space=pltpu.SMEM)]
        scratch += [*GATHER_SEMS, pltpu.VMEM((D, F), f32), pltpu.VMEM((F, D), f32)]
    else:
        shapes = [((LAYERS, D, F), bf16), ((LAYERS, F, D), bf16), acts]
        out_specs = [ANY] * 3
        scratch += [*GATHER_SEMS, pltpu.VMEM((2, D, F), f32), pltpu.VMEM((2, F, D), f32), DMA((2, 2))]
    options = dict(
        out_shape=[jax.ShapeDtypeStruct(*s) for s in shapes],
        in_specs=[V, V, ANY, ANY] + [ANY] * len(pert),
        out_specs=out_specs,
        scratch_shapes=scratch,
        compiler_params=pltpu.CompilerParams(
            collective_id=1 if perturbed else 0, has_side_effects=True, vmem_limit_bytes=VMEM_LIMIT),
        name="second_pass" if perturbed else "first_pass",
    )
    kernel = functools.partial(pass_kernel, perturbed, inv_count, radius)
    if perturbed:
        return pl.pallas_call(kernel, **options)(x, y, w_in, w_out, *pert)
    return pl.pallas_call(kernel, **options)(x, y, w_in, w_out)


def solution(mesh):
    mesh_axes = tuple(mesh.axis_names)
    dev_count = math.prod([mesh.shape[axis_name] for axis_name in mesh_axes])
    batch_spec = P(mesh_axes, None, None)

    def local_step(images, targets, w_in, w_out):
        layers, model_dim, hidden_dim = w_in.shape
        inv_count = 1.0 / (images.shape[0] * images.shape[1] * dev_count * model_dim)
        radius = RHO_REL * math.sqrt(layers * hidden_dim + model_dim)
        x, y = images.reshape(T, D), targets.reshape(T, D)
        pert = one_pass(False, inv_count, radius, x, y, w_in, w_out)[:2]
        new_in, new_out, _, loss = one_pass(True, inv_count, radius, x, y, w_in, w_out, pert)
        return new_in, new_out, loss.reshape(())

    return jax.shard_map(local_step, mesh=mesh, in_specs=(batch_spec, batch_spec, P(), P()), out_specs=(P(), P(), P()), check_vma=False)
```
